8 devices in a mesh: dp: 2 (over z, y), ep: 4 (over x, core).
Axes of the slice: x: 2, y: 2, z: 1, core: 2. Of those that a mesh axis runs over, the one named last changes fastest.
Arguments:
- x_in: bfloat16 [8192, 4096], P(('dp', 'ep'))
- ln_gain: float32 [4096], replicated
- ln_bias: float32 [4096], replicated
- w_router: bfloat16 [4096, 16], replicated
- w_gate: bfloat16 [16, 4096, 688], P('ep')
- w_up: bfloat16 [16, 4096, 688], P('ep')
- w_down: bfloat16 [16, 688, 4096], P('ep')
- expert_ids: int32 [8192, 2], P(('dp', 'ep'))
- slot_ids: int32 [8192, 2], P(('dp', 'ep'))
- d_out: bfloat16 [8192, 4096], P(('dp', 'ep'))
Outputs:
- output 1: bfloat16 [8192, 4096], P(('dp', 'ep'))
- output 2: bfloat16 [8192, 4096], P(('dp', 'ep'))
- output 3: float32 [4096], replicated
- output 4: float32 [4096], replicated
- output 5: float32 [4096, 16], replicated
- output 6: float32 [16, 4096, 688], P('ep')
- output 7: float32 [16, 4096, 688], P('ep')
- output 8: float32 [16, 688, 4096], P('ep')
All inputs are finite; a program needn't handle non-finite values.
Results may differ from the reference program's by a relative error of at most 0.00541992.
Values are sent between devices in bfloat16 or wider.
A program may use at most 1 GiB of HBM per device.

```python
import jax
import jax.numpy as jnp
from jax import lax

D = 4096
FF = 688
EXPERTS = 16
TOP = 2
TOKENS_DEV = 1024
DEVICES = 8
CAPACITY = 160
TOKENS = DEVICES * TOKENS_DEV
SLOT_ROWS = EXPERTS * CAPACITY
LN_EPS = 1e-5


def draw_routing(key_route):
    key_hot, key_perm, key_first, key_shift = jax.random.split(key_route, 4)
    hot_expert = jax.random.randint(key_hot, (DEVICES, 1), 0, EXPERTS)
    perm_keys = jax.random.split(key_perm, DEVICES)
    perm_pos = jax.vmap(lambda key_one: jax.random.permutation(key_one, TOKENS_DEV))(perm_keys)
    forced = perm_pos < (3 * CAPACITY) // 2
    first_pick = jax.random.randint(key_first, (DEVICES, TOKENS_DEV), 0, EXPERTS)
    first_pick = jnp.where(forced, hot_expert, first_pick)
    shift_by = jax.random.randint(key_shift, (DEVICES, TOKENS_DEV), 1, EXPERTS)
    second_pick = (first_pick + shift_by) % EXPERTS
    choice = jnp.stack([first_pick, second_pick], axis=-1)
    flat_pick = choice.reshape(DEVICES, TOKENS_DEV * TOP)
    onehot = (flat_pick[:, :, None] == jnp.arange(EXPERTS)[None, None, :]).astype(jnp.int32)
    before = jnp.cumsum(onehot, axis=1) - onehot
    pair_rank = jnp.sum(before * onehot, axis=-1)
    slot_pos = jnp.where(pair_rank < CAPACITY, pair_rank, -1)
    return choice.reshape(TOKENS, TOP).astype(jnp.int32), slot_pos.reshape(TOKENS, TOP).astype(jnp.int32)


def setup_inputs(seed: int = 0) -> dict:
    key_root = jax.random.key(seed)
    key_list = jax.random.split(key_root, 10)
    x_in = jax.random.normal(key_list[0], (TOKENS, D), jnp.float32).astype(jnp.bfloat16)
    ln_gain = 1.0 + 0.3 * jax.random.normal(key_list[1], (D,), jnp.float32)
    ln_bias = 0.3 * jax.random.normal(key_list[2], (D,), jnp.float32)
    w_router = (jax.random.normal(key_list[3], (D, EXPERTS), jnp.float32) * D ** -0.5).astype(jnp.bfloat16)
    w_gate = (jax.random.normal(key_list[4], (EXPERTS, D, FF), jnp.float32) * D ** -0.5).astype(jnp.bfloat16)
    w_up = (jax.random.normal(key_list[5], (EXPERTS, D, FF), jnp.float32) * D ** -0.5).astype(jnp.bfloat16)
    w_down = (jax.random.normal(key_list[6], (EXPERTS, FF, D), jnp.float32) * (2.0 * FF ** -0.5)).astype(jnp.bfloat16)
    expert_ids, slot_ids = draw_routing(key_list[7])
    d_out = jax.random.normal(key_list[8], (TOKENS, D), jnp.float32).astype(jnp.bfloat16)
    return {"x_in": x_in, "ln_gain": ln_gain, "ln_bias": ln_bias, "w_router": w_router, "w_gate": w_gate, "w_up": w_up, "w_down": w_down, "expert_ids": expert_ids, "slot_ids": slot_ids, "d_out": d_out}


def to_bf16_grid(array_in):
    return array_in.astype(jnp.bfloat16).astype(jnp.float32)


def reference(x_in, ln_gain, ln_bias, w_router, w_gate, w_up, w_down, expert_ids, slot_ids, d_out):
    ids_dev = expert_ids.reshape(DEVICES, TOKENS_DEV, TOP)
    slots_dev = slot_ids.reshape(DEVICES, TOKENS_DEV, TOP)
    target = jnp.where(slots_dev >= 0, ids_dev * CAPACITY + slots_dev, -1)
    pair_hot = (target[..., None] == jnp.arange(SLOT_ROWS)).astype(jnp.float32)
    token_hot = jnp.sum(pair_hot, axis=2)

    def block_fn(x_f, gain_vec, bias_vec, router_f, gate_f, up_f, down_f):
        x_dev = x_f.reshape(DEVICES, TOKENS_DEV, D)
        mean_x = jnp.mean(x_dev, axis=-1, keepdims=True)
        centered = x_dev - mean_x
        var_x = jnp.mean(centered * centered, axis=-1, keepdims=True)
        normed = centered * lax.rsqrt(var_x + LN_EPS)
        hidden = to_bf16_grid(normed * gain_vec + bias_vec)
        logits = jnp.einsum("dtm,me->dte", hidden, router_f)
        gate_probs = jax.nn.softmax(jnp.take_along_axis(logits, ids_dev, axis=-1), axis=-1)
        buffers = to_bf16_grid(jnp.einsum("dts,dtm->dsm", token_hot, hidden))
        buffers = buffers.reshape(DEVICES, EXPERTS, CAPACITY, D)
        act_gate = to_bf16_grid(jnp.einsum("decm,emf->decf", buffers, gate_f))
        act_up = to_bf16_grid(jnp.einsum("decm,emf->decf", buffers, up_f))
        act_mix = to_bf16_grid(jax.nn.silu(act_gate) * act_up)
        expert_out = to_bf16_grid(jnp.einsum("decf,efm->decm", act_mix, down_f))
        pair_out = jnp.einsum("dtks,dsm->dtkm", pair_hot, expert_out.reshape(DEVICES, SLOT_ROWS, D))
        mixed = jnp.einsum("dtk,dtkm->dtm", gate_probs, pair_out)
        return to_bf16_grid(x_dev + mixed).reshape(TOKENS, D)

    moe_f, pullback = jax.vjp(block_fn, x_in.astype(jnp.float32), ln_gain, ln_bias, w_router.astype(jnp.float32), w_gate.astype(jnp.float32), w_up.astype(jnp.float32), w_down.astype(jnp.float32))
    grad_list = pullback(d_out.astype(jnp.float32))
    return (moe_f.astype(jnp.bfloat16), grad_list[0].astype(jnp.bfloat16), grad_list[1], grad_list[2], grad_list[3], grad_list[4], grad_list[5], grad_list[6])
```

```python
import functools

import jax
import jax.numpy as jnp
from jax import lax
from jax.experimental import pallas as pl
from jax.experimental.pallas import tpu as pltpu
from jax.sharding import PartitionSpec as P


LN_EPS = 1e-5
F32 = jnp.float32
BF16 = jnp.bfloat16
VMEM_LIMIT = 62 * 1024 * 1024


def capacity_for(tokens_dev, experts, n_top):
    return 8 * ((5 * tokens_dev * n_top + 32 * experts - 1) // (32 * experts))


def params(n_axes):
    return pltpu.CompilerParams(dimension_semantics=("arbitrary",) * n_axes, vmem_limit_bytes=VMEM_LIMIT)


def cost(flops, nbytes):
    return pl.CostEstimate(flops=int(flops), bytes_accessed=int(nbytes), transcendentals=0)


def dot_nn(lhs, rhs):
    return lax.dot_general(lhs, rhs, (((1,), (0,)), ((), ())), preferred_element_type=F32)


def dot_nt(lhs, rhs):
    return lax.dot_general(lhs, rhs, (((1,), (1,)), ((), ())), preferred_element_type=F32)


def dot_tn(lhs, rhs):
    return lax.dot_general(lhs, rhs, (((0,), (0,)), ((), ())), preferred_element_type=F32)


def gather_body(n_src, scaled, *refs):
    tok_ref = refs[0]
    p_ref = refs[1] if scaled else None
    srcs = refs[1 + scaled:1 + scaled + n_src]
    out_ref, hot = refs[1 + scaled + n_src:]
    r = pl.program_id(0)
    tokens = hot.shape[1]

    @pl.when(pl.program_id(1) == 0)
    def _():
        lanes = lax.broadcasted_iota(jnp.int32, (hot.shape[0], tokens), 1)
        hot[...] = (tok_ref[0] == lanes).astype(F32).astype(BF16)

    for q in range(n_src):
        @pl.when(r == q)
        def _():
            rows = dot_nn(hot[...], srcs[q][...])
            if scaled:
                rows = rows * p_ref[0]
            out_ref[...] = rows.astype(BF16).reshape(out_ref.shape)


def gather_rows(tok, p_slot, sources, local_exp, tile=2048):
    n_src = len(sources)
    tokens, dim = sources[0].shape
    slots = tok.shape[1]
    cap = slots // local_exp
    scaled = p_slot is not None
    n_tiles = dim // tile
    col = pl.BlockSpec((1, slots, 1), lambda r, n: (r, 0, 0))

    def src_map(q, r, n):
        return (0, jnp.where(r == q, n, jnp.where(r < q, 0, n_tiles - 1)))

    args = (tok,) + ((p_slot,) if scaled else ()) + tuple(sources)
    return pl.pallas_call(
        functools.partial(gather_body, n_src, scaled),
        grid=(n_src, n_tiles),
        in_specs=[col] * (1 + scaled) + [pl.BlockSpec((tokens, tile), functools.partial(src_map, q)) for q in range(n_src)],
        out_specs=pl.BlockSpec((local_exp, cap, tile), lambda r, n: (0, r, n)),
        out_shape=jax.ShapeDtypeStruct((local_exp, n_src * cap, dim), BF16),
        scratch_shapes=[pltpu.VMEM((slots, tokens), BF16)],
        compiler_params=params(2),
        cost_estimate=cost(2 * n_src * slots * tokens * dim, 2 * n_src * (tokens + slots) * dim),
        name="gather_rows",
    )(*args)


def act_forward(rows, gate, up):
    pre_gate = dot_nt(rows, gate).astype(BF16)
    pre_up = dot_nt(rows, up).astype(BF16)
    gate_f = pre_gate.astype(F32)
    act_mix = (gate_f * jax.nn.sigmoid(gate_f) * pre_up.astype(F32)).astype(BF16)
    return pre_gate, pre_up, act_mix


def act_backward(d_mix, pre_gate, pre_up):
    d_mix = d_mix.astype(BF16).astype(F32)
    gate_f = pre_gate.astype(F32)
    sig = jax.nn.sigmoid(gate_f)
    d_gate = (d_mix * pre_up.astype(F32) * sig * (1.0 + gate_f * (1.0 - sig))).astype(BF16)
    d_up = (d_mix * gate_f * sig).astype(BF16)
    return d_gate, d_up


def store_halves(lo_ref, hi_ref, cols, value):
    half = lo_ref.shape[1]
    lo_ref[0, :, cols] = value[:half].astype(BF16)
    hi_ref[0, :, cols] = value[half:].astype(BF16)


def forward_body(tile, rows_ref, gate_ref, up_ref, down_ref, a_ref, u_ref, m_ref, lo_ref, hi_ref):
    pre_gate, pre_up, act_mix = act_forward(rows_ref[0], gate_ref[0], up_ref[0])
    a_ref[0] = pre_gate
    u_ref[0] = pre_up
    m_ref[0] = act_mix
    for n in range(lo_ref.shape[-1] // tile):
        cols = pl.ds(n * tile, tile)
        store_halves(lo_ref, hi_ref, cols, dot_nn(act_mix, down_ref[0, :, cols]))


def backward_body(tile, rows_ref, a_ref, u_ref, gate_ref, up_ref, down_ref, dg_ref, du_ref, lo_ref, hi_ref):
    d_gate, d_up = act_backward(dot_nt(rows_ref[0], down_ref[0]), a_ref[0], u_ref[0])
    dg_ref[0] = d_gate
    du_ref[0] = d_up
    for n in range(lo_ref.shape[-1] // tile):
        cols = pl.ds(n * tile, tile)
        store_halves(lo_ref, hi_ref, cols, dot_nn(d_gate, gate_ref[0, :, cols]) + dot_nn(d_up, up_ref[0, :, cols]))


def both_body(rows_ref, grad_ref, gate_ref, up_ref, down_ref, m_ref, dg_ref, du_ref):
    pre_gate, pre_up, act_mix = act_forward(rows_ref[0], gate_ref[0], up_ref[0])
    m_ref[0] = act_mix
    d_gate, d_up = act_backward(dot_nt(grad_ref[0], down_ref[0]), pre_gate, pre_up)
    dg_ref[0] = d_gate
    du_ref[0] = d_up


def expert_forward(rows, gate_t, up_t, down):
    n_exp, n_rows, dim = rows.shape
    ff = down.shape[1]
    w_spec = pl.BlockSpec((1, ff, dim), lambda e: (e, 0, 0))
    r_spec = pl.BlockSpec((1, n_rows, dim), lambda e: (e, 0, 0))
    f_spec = pl.BlockSpec((1, n_rows, ff), lambda e: (e, 0, 0))
    f_shape = jax.ShapeDtypeStruct((n_exp, n_rows, ff), BF16)
    h_spec = pl.BlockSpec((1, n_rows // 2, dim), lambda e: (e, 0, 0))
    h_shape = jax.ShapeDtypeStruct((n_exp, n_rows // 2, dim), BF16)
    return pl.pallas_call(
        functools.partial(forward_body, 1024),
        grid=(n_exp,),
        in_specs=[r_spec, w_spec, w_spec, w_spec],
        out_specs=[f_spec, f_spec, f_spec, h_spec, h_spec],
        out_shape=[f_shape, f_shape, f_shape, h_shape, h_shape],
        compiler_params=params(1),
        cost_estimate=cost(6 * n_exp * n_rows * dim * ff, 2 * n_exp * (3 * ff * dim + 2 * n_rows * dim)),
        name="expert_forward",
    )(rows, gate_t, up_t, down)


def expert_backward(rows, a, u, gate_t, up_t, down):
    n_exp, n_rows, dim = rows.shape
    ff = down.shape[1]
    w_spec = pl.BlockSpec((1, ff, dim), lambda e: (e, 0, 0))
    r_spec = pl.BlockSpec((1, n_rows, dim), lambda e: (e, 0, 0))
    f_spec = pl.BlockSpec((1, n_rows, ff), lambda e: (e, 0, 0))
    f_shape = jax.ShapeDtypeStruct((n_exp, n_rows, ff), BF16)
    h_spec = pl.BlockSpec((1, n_rows // 2, dim), lambda e: (e, 0, 0))
    h_shape = jax.ShapeDtypeStruct((n_exp, n_rows // 2, dim), BF16)
    return pl.pallas_call(
        functools.partial(backward_body, 1024),
        grid=(n_exp,),
        in_specs=[r_spec, f_spec, f_spec, w_spec, w_spec, w_spec],
        out_specs=[f_spec, f_spec, h_spec, h_spec],
        out_shape=[f_shape, f_shape, h_shape, h_shape],
        compiler_params=params(1),
        cost_estimate=cost(6 * n_exp * n_rows * dim * ff, 2 * n_exp * (3 * ff * dim + 2 * n_rows * dim)),
        name="expert_backward",
    )(rows, a, u, gate_t, up_t, down)


def expert_both(rows, grads, gate_t, up_t, down, splits=2):
    n_exp, n_rows, dim = rows.shape
    ff = down.shape[1]
    part = n_rows // splits
    w_spec = pl.BlockSpec((1, ff, dim), lambda e, s: (e, 0, 0))
    r_spec = pl.BlockSpec((1, part, dim), lambda e, s: (e, s, 0))
    f_spec = pl.BlockSpec((1, part, ff), lambda e, s: (e, s, 0))
    f_shape = jax.ShapeDtypeStruct((n_exp, n_rows, ff), BF16)
    return pl.pallas_call(
        both_body,
        grid=(n_exp, splits),
        in_specs=[r_spec, r_spec, w_spec, w_spec, w_spec],
        out_specs=[f_spec] * 3,
        out_shape=[f_shape] * 3,
        compiler_params=params(2),
        cost_estimate=cost(6 * n_exp * n_rows * dim * ff, 2 * n_exp * (3 * ff * dim + 2 * n_rows * dim)),
        name="expert_both",
    )(rows, grads, gate_t, up_t, down)


def wgrad_body(n_parts, *refs):
    small, wide = refs[:n_parts], refs[n_parts:2 * n_parts]
    out_ref, small_all, wide_all = refs[2 * n_parts:]
    start = 0
    for part in range(n_parts):
        span = pl.ds(start, small[part].shape[1])
        start += small[part].shape[1]

        @pl.when(pl.program_id(1) == 0)
        def _():
            small_all[span, :] = small[part][0]

        wide_all[span, :] = wide[part][0]
    out_ref[0] = dot_tn(small_all[...], wide_all[...])


def weight_grad(small, wide, tile=1024):
    n_exp, _, ff = small[0].shape
    dim = wide[0].shape[2]
    total = sum(s.shape[1] for s in small)
    return pl.pallas_call(
        functools.partial(wgrad_body, len(small)),
        grid=(n_exp, dim // tile),
        in_specs=[pl.BlockSpec((1, s.shape[1], ff), lambda e, n: (e, 0, 0)) for s in small]
        + [pl.BlockSpec((1, w.shape[1], tile), lambda e, n: (e, 0, n)) for w in wide],
        out_specs=pl.BlockSpec((1, ff, tile), lambda e, n: (e, 0, n)),
        out_shape=jax.ShapeDtypeStruct((n_exp, ff, dim), F32),
        scratch_shapes=[pltpu.VMEM((total, ff), BF16), pltpu.VMEM((total, tile), BF16)],
        compiler_params=params(2),
        cost_estimate=cost(2 * n_exp * total * dim * ff, n_exp * (4 * ff * dim + 2 * total * (dim + ff))),
        name="weight_grad",
    )(*small, *wide)


def fill_hot(tgt_ref, *hots):
    chunk = 128
    slots = hots[0].shape[1]

    @pl.loop(0, hots[0].shape[0] // chunk)
    def _(c):
        rows = pl.ds(pl.multiple_of(c * chunk, chunk), chunk)
        lanes = lax.broadcasted_iota(jnp.int32, (chunk, slots), 1)
        first, second = tgt_ref[rows, 0:1] == lanes, tgt_ref[rows, 1:2] == lanes
        if len(hots) == 2:
            hots[0][rows, :] = first.astype(F32).astype(BF16)
            hots[1][rows, :] = second.astype(F32).astype(BF16)
        else:
            hots[0][rows, :] = (first | second).astype(F32).astype(BF16)


def combine_body(n_ret, tgt_ref, p_ref, x_ref, dout_ref, *refs):
    rets = refs[:n_ret]
    out_ref, dgate_ref, hot_a, hot_b, rows = refs[n_ret:]

    @pl.when(pl.program_id(0) == 0)
    def _():
        fill_hot(tgt_ref, hot_a, hot_b)
        dgate_ref[...] = jnp.zeros_like(dgate_ref)

    n_exp, cap, tile = rets[0].shape
    for q in range(n_ret):
        rows[pl.ds(q * n_exp * cap, n_exp * cap), :] = rets[q][...].reshape(n_exp * cap, tile)
    first = dot_nn(hot_a[...], rows[...])
    second = dot_nn(hot_b[...], rows[...])
    dout = dout_ref[...].astype(F32)
    out_ref[...] = (x_ref[...].astype(F32) + (p_ref[:, 0:1] * first + p_ref[:, 1:2] * second)).astype(BF16)
    dgate_ref[:, 0:1] += jnp.sum(first * dout, axis=1, keepdims=True)
    dgate_ref[:, 1:2] += jnp.sum(second * dout, axis=1, keepdims=True)


def combine(tgt, gate_probs, x_loc, dout, rets, tile=512):
    tokens, dim = x_loc.shape
    n_exp, cap, _ = rets[0].shape
    slots = len(rets) * n_exp * cap
    full = pl.BlockSpec((tokens, 2), lambda n: (0, 0))
    cols = pl.BlockSpec((tokens, tile), lambda n: (0, n))
    return pl.pallas_call(
        functools.partial(combine_body, len(rets)),
        grid=(dim // tile,),
        in_specs=[full, full, cols, cols] + [pl.BlockSpec((n_exp, cap, tile), lambda n: (0, 0, n))] * len(rets),
        out_specs=[cols, full],
        out_shape=[jax.ShapeDtypeStruct((tokens, dim), BF16), jax.ShapeDtypeStruct((tokens, 2), F32)],
        scratch_shapes=[pltpu.VMEM((tokens, slots), BF16), pltpu.VMEM((tokens, slots), BF16), pltpu.VMEM((slots, tile), BF16)],
        compiler_params=params(1),
        cost_estimate=cost(4 * tokens * slots * dim, 2 * (3 * tokens + slots) * dim),
        name="combine",
    )(tgt, gate_probs, x_loc, dout, *rets)


def finish_body(n_ret, tgt_ref, dlog_ref, stat_ref, router_ref, gain_ref, x_ref, dout_ref, *refs):
    rets = refs[:n_ret]
    gx_ref, ggain_ref, gbias_ref, hot, rows, d_hid, row_sums = refs[n_ret:]
    phase, n = pl.program_id(0), pl.program_id(1)
    n_exp, cap, tile = rets[0].shape
    dim = d_hid.shape[1]
    cols = pl.ds(pl.multiple_of(n * tile, tile), tile)

    @pl.when((phase == 0) & (n == 0))
    def _():
        fill_hot(tgt_ref, hot)
        row_sums[...] = jnp.zeros_like(row_sums)

    inv_std = stat_ref[:, 1:2]
    normed = (x_ref[...].astype(F32) - stat_ref[:, 0:1]) * inv_std

    @pl.when(phase == 0)
    def _():
        for q in range(n_ret):
            rows[pl.ds(q * n_exp * cap, n_exp * cap), :] = rets[q][...].reshape(n_exp * cap, tile)
        total = dot_nn(hot[...], rows[...]) + dot_nn(dlog_ref[...], router_ref[...])
        rounded = total.astype(BF16)
        d_hid[:, cols] = rounded
        d_h = rounded.astype(F32)
        weighted = d_h * normed
        ggain_ref[...] = jnp.sum(weighted, axis=0, keepdims=True)
        gbias_ref[...] = jnp.sum(d_h, axis=0, keepdims=True)
        row_sums[:, 0:1] += jnp.sum(d_h * gain_ref[...], axis=1, keepdims=True)
        row_sums[:, 1:2] += jnp.sum(weighted * gain_ref[...], axis=1, keepdims=True)

    @pl.when(phase == 1)
    def _():
        d_norm = d_hid[:, cols].astype(F32) * gain_ref[...]
        mean_dn = row_sums[:, 0:1] * (1.0 / dim)
        mean_dnn = row_sums[:, 1:2] * (1.0 / dim)
        gx_ref[...] = (dout_ref[...].astype(F32) + inv_std * (d_norm - mean_dn - normed * mean_dnn)).astype(BF16)


def finish(tgt, d_logits, stats, router_t, gain, x_loc, dout, rets, tile=512):
    tokens, dim = x_loc.shape
    experts = d_logits.shape[1]
    n_exp, cap, _ = rets[0].shape
    slots = len(rets) * n_exp * cap
    last = dim // tile - 1
    full = pl.BlockSpec((tokens, 2), lambda p, n: (0, 0))
    both = pl.BlockSpec((tokens, tile), lambda p, n: (0, n))
    late = pl.BlockSpec((tokens, tile), lambda p, n: (0, n * p))
    line = pl.BlockSpec((1, tile), lambda p, n: (0, n))
    early_line = pl.BlockSpec((1, tile), lambda p, n: (0, jnp.where(p == 0, n, last)))

    ret_spec = pl.BlockSpec((n_exp, cap, tile), lambda p, n: (0, 0, jnp.where(p == 0, n, last)))
    return pl.pallas_call(
        functools.partial(finish_body, len(rets)),
        grid=(2, dim // tile),
        in_specs=[full, pl.BlockSpec((tokens, experts), lambda p, n: (0, 0)), full, pl.BlockSpec((experts, tile), lambda p, n: (0, n)), line, both, late]
        + [ret_spec] * len(rets),
        out_specs=[late, early_line, early_line],
        out_shape=[jax.ShapeDtypeStruct((tokens, dim), BF16), jax.ShapeDtypeStruct((1, dim), F32), jax.ShapeDtypeStruct((1, dim), F32)],
        scratch_shapes=[pltpu.VMEM((tokens, slots), BF16), pltpu.VMEM((slots, tile), BF16), pltpu.VMEM((tokens, dim), BF16), pltpu.VMEM((tokens, 2), F32)],
        compiler_params=params(2),
        cost_estimate=cost(2 * tokens * slots * dim, 2 * (5 * tokens + slots) * dim),
        name="finish",
    )(tgt, d_logits, stats, router_t, gain, x_loc, dout, *rets)


def after(value, *earlier):
    return lax.optimization_barrier((value,) + earlier)[0]


def solution(mesh):
    n_dp, n_ep = mesh.shape["dp"], mesh.shape["ep"]
    tok_spec = P(("dp", "ep"), None)
    exp_spec = P("ep", None, None)

    def swap(value, bits):
        return lax.ppermute(value, "ep", [(j, j ^ bits) for j in range(n_ep)])

    def cross(value):
        return lax.ppermute(value, "dp", [(i, i ^ 1) for i in range(n_dp)])

    def local_step(x_loc, ln_gain, ln_bias, w_router, w_gate, w_up, w_down, ids_loc, slots_loc, dout):
        tokens, _ = x_loc.shape
        experts = w_router.shape[1]
        n_exp = w_gate.shape[0]
        n_top = ids_loc.shape[1]
        cap = capacity_for(tokens, experts, n_top)
        local = n_exp * cap
        i, j = lax.axis_index("dp"), lax.axis_index("ep")
        gate_t, up_t = jnp.swapaxes(w_gate, 1, 2), jnp.swapaxes(w_up, 1, 2)

        x_f = x_loc.astype(F32)
        mean_x = jnp.mean(x_f, axis=-1, keepdims=True)
        centered = x_f - mean_x
        var_x = jnp.mean(centered * centered, axis=-1, keepdims=True)
        inv_std = lax.rsqrt(var_x + LN_EPS)
        hidden = (centered * inv_std * ln_gain + ln_bias).astype(BF16)
        h_x = swap(hidden, 2)
        h_c = swap(hidden, 1)
        g_0 = cross(hidden)
        logits = jnp.dot(hidden, w_router, preferred_element_type=F32)
        pick_mask = (ids_loc[..., None] == jnp.arange(experts)).astype(F32)
        gate_probs = jax.nn.softmax(jnp.sum(pick_mask * logits[..., None, :], axis=-1), axis=-1)

        kept = slots_loc >= 0
        target = jnp.where(kept, ids_loc * cap + slots_loc, -1)
        match = target[None, :, :] == jnp.arange(experts * cap)[:, None, None]
        token_no = jnp.arange(tokens, dtype=F32)[None, :, None]
        tok_slot = jnp.sum(jnp.where(match, token_no + 1.0, 0.0), axis=(1, 2)) - 1.0
        p_slot = jnp.sum(jnp.where(match, gate_probs[None], 0.0), axis=(1, 2))
        tables = jnp.stack([tok_slot, p_slot])
        d_late = after(dout, tables)
        tables = lax.all_gather(tables, ("dp", "ep"))
        tables = lax.dynamic_slice_in_dim(tables, j * local, local, axis=2)

        def table_of(dp_idx, rels):
            rows = [lax.dynamic_index_in_dim(tables, dp_idx * n_ep + (j ^ r), 0, keepdims=False) for r in rels]
            part = jnp.stack(rows)
            return part[:, 0].astype(jnp.int32)[..., None], part[:, 1][..., None]

        tok_a, p_a = table_of(i, (0, 1))
        tok_b, p_b = table_of(i, (2, 3))
        tok_o, p_o = table_of(1 - i, (0, 1))
        tok_q, p_q = table_of(1 - i, (2, 3))

        d_x = swap(d_late, 2)
        d_c = swap(d_late, 1)
        e_0 = cross(d_late)
        rows_a = gather_rows(tok_a, None, (hidden, h_c), n_exp)
        act_a = expert_forward(rows_a, gate_t, up_t, w_down)
        grads_a = gather_rows(tok_a, p_a, (dout, d_c), n_exp)
        back_a = expert_backward(grads_a, act_a[0], act_a[1], gate_t, up_t, w_down)

        h_xc = swap(h_x, 1)
        g_2 = cross(h_x)
        rows_b = gather_rows(tok_b, None, (h_x, h_xc), n_exp)
        act_b = expert_forward(rows_b, gate_t, up_t, w_down)
        y_home = [act_a[3], swap(act_a[4], 1), swap(act_b[3], 2), swap(act_b[4], 3)]
        d_xc = swap(d_x, 1)
        e_2 = cross(d_x)
        grads_b = gather_rows(tok_b, p_b, (d_x, d_xc), n_exp)
        back_b = expert_backward(grads_b, act_b[0], act_b[1], gate_t, up_t, w_down)
        d_home = [back_a[2], swap(back_a[3], 1), swap(back_b[2], 2), swap(back_b[3], 3)]

        g_1, g_3 = swap(g_0, 1), swap(g_2, 1)
        e_1, e_3 = swap(e_0, 1), swap(e_2, 1)
        rows_o = gather_rows(tok_o, None, (g_0, g_1), n_exp)
        grads_o = gather_rows(tok_o, p_o, (e_0, e_1), n_exp)
        mix_o, dg_o, du_o = expert_both(rows_o, grads_o, gate_t, up_t, w_down, 1)
        rows_q = gather_rows(tok_q, None, (g_2, g_3), n_exp)
        grads_q = gather_rows(tok_q, p_q, (e_2, e_3), n_exp)
        mix_q, dg_q, du_q = expert_both(rows_q, grads_q, gate_t, up_t, w_down, 1)
        wide_h, wide_d = (rows_a, rows_b, rows_o, rows_q), (grads_a, grads_b, grads_o, grads_q)
        grad_down = weight_grad((act_a[2], act_b[2], mix_o, mix_q), wide_d)
        grad_gate = weight_grad((back_a[0], back_b[0], dg_o, dg_q), wide_h)
        grad_up = weight_grad((back_a[1], back_b[1], du_o, du_q), wide_h)

        owner = ids_loc // n_exp
        tgt = jnp.where(kept, (owner ^ j) * local + (ids_loc % n_exp) * cap + slots_loc, -1)
        moe_out, d_gates = combine(tgt, gate_probs, x_loc, dout, y_home)
        d_chosen = gate_probs * (d_gates - jnp.sum(gate_probs * d_gates, axis=-1, keepdims=True))
        d_logits = jnp.sum(d_chosen[..., None] * pick_mask, axis=-2)
        grad_router = lax.psum(jnp.einsum("tm,te->me", hidden, d_logits, preferred_element_type=F32), ("dp", "ep"))
        stats = jnp.concatenate([mean_x, inv_std], axis=1)
        grad_x, g_gain, g_bias = finish(tgt, d_logits.astype(BF16), stats, w_router.T, ln_gain[None], x_loc, dout, d_home)
        g_gain, g_bias = lax.psum((g_gain[0], g_bias[0]), ("dp", "ep"))
        return (moe_out, grad_x, g_gain, g_bias, grad_router, jnp.swapaxes(grad_gate, 1, 2), jnp.swapaxes(grad_up, 1, 2), grad_down)

    return jax.shard_map(local_step, mesh=mesh, in_specs=(tok_spec, P(None), P(None), P(None, None), exp_spec, exp_spec, exp_spec, tok_spec, tok_spec, tok_spec), out_specs=(tok_spec, tok_spec, P(None), P(None), P(None, None), exp_spec, exp_spec, exp_spec), check_vma=False)
```

```python
import functools

import jax
import jax.numpy as jnp
from jax import lax
from jax.experimental import pallas as pl
from jax.experimental.pallas import tpu as pltpu
from jax.sharding import PartitionSpec as P


LN_EPS = 1e-5
F32 = jnp.float32
BF16 = jnp.bfloat16
VMEM_LIMIT = 62 * 1024 * 1024


def capacity_for(tokens_dev, experts, n_top):
    return 8 * ((5 * tokens_dev * n_top + 32 * experts - 1) // (32 * experts))


def params(n_axes):
    return pltpu.CompilerParams(dimension_semantics=("arbitrary",) * n_axes, vmem_limit_bytes=VMEM_LIMIT)


def cost(flops, nbytes):
    return pl.CostEstimate(flops=int(flops), bytes_accessed=int(nbytes), transcendentals=0)


def dot_nn(lhs, rhs):
    return lax.dot_general(lhs, rhs, (((1,), (0,)), ((), ())), preferred_element_type=F32)


def dot_nt(lhs, rhs):
    return lax.dot_general(lhs, rhs, (((1,), (1,)), ((), ())), preferred_element_type=F32)


def dot_tn(lhs, rhs):
    return lax.dot_general(lhs, rhs, (((0,), (0,)), ((), ())), preferred_element_type=F32)


def norm_body(x_ref, gain_ref, bias_ref, router_ref, hid_ref, stat_ref, logit_ref):
    x_f = x_ref[...].astype(F32)
    mean = jnp.mean(x_f, axis=-1, keepdims=True)
    centered = x_f - mean
    inv_std = lax.rsqrt(jnp.mean(centered * centered, axis=-1, keepdims=True) + LN_EPS)
    hidden = (centered * inv_std * gain_ref[...] + bias_ref[...]).astype(BF16)
    hid_ref[...] = hidden
    stat_ref[:, 0:1] = mean
    stat_ref[:, 1:2] = inv_std
    logit_ref[...] = dot_nt(hidden, router_ref[...])


def norm_router(x_loc, gain, bias, router_t, tile=256):
    tokens, dim = x_loc.shape
    experts = router_t.shape[0]
    line = pl.BlockSpec((1, dim), lambda t: (0, 0))
    return pl.pallas_call(
        norm_body,
        grid=(tokens // tile,),
        in_specs=[pl.BlockSpec((tile, dim), lambda t: (t, 0)), line, line, pl.BlockSpec((experts, dim), lambda t: (0, 0))],
        out_specs=[pl.BlockSpec((tile, dim), lambda t: (t, 0)), pl.BlockSpec((tile, 2), lambda t: (t, 0)), pl.BlockSpec((tile, experts), lambda t: (t, 0))],
        out_shape=[jax.ShapeDtypeStruct((tokens, dim), BF16), jax.ShapeDtypeStruct((tokens, 2), F32), jax.ShapeDtypeStruct((tokens, experts), F32)],
        compiler_params=params(1),
        cost_estimate=cost(20 * tokens * dim, 4 * tokens * dim),
        name="norm_router",
    )(x_loc, gain, bias, router_t)


def gather_body(n_src, scaled, base_ref, *refs):
    routes, srcs = refs[:n_src], refs[n_src:2 * n_src]
    out_ref, hot, p_col = refs[2 * n_src:]
    r, n = pl.program_id(0), pl.program_id(1)
    n_exp, cap, _ = out_ref.shape
    tokens = hot.shape[1]

    for q in range(n_src):
        @pl.when((r == q) & (n == 0))
        def _():
            for e in range(n_exp):
                span = pl.ds(e * cap, cap)
                slot = (lax.broadcasted_iota(jnp.int32, (cap, tokens), 0) + (base_ref[0] + e * cap)).astype(F32)
                first, second = routes[q][0:1, :] == slot, routes[q][1:2, :] == slot
                hot[span, :] = (first | second).astype(F32).astype(BF16)
                if scaled:
                    chosen = jnp.where(first, routes[q][2:3, :], jnp.where(second, routes[q][3:4, :], 0.0))
                    p_col[span, :] = jnp.sum(chosen, axis=1, keepdims=True)

        @pl.when(r == q)
        def _():
            rows = dot_nn(hot[...], srcs[q][...])
            if scaled:
                rows = rows * p_col[...]
            out_ref[...] = rows.astype(BF16).reshape(out_ref.shape)


def gather_rows(base, routes, sources, n_exp, cap, scaled, tile=2048):
    n_src = len(sources)
    tokens, dim = sources[0].shape
    tile = min(tile, dim)
    slots = n_exp * cap
    n_tiles = dim // tile

    def src_map(q, r, n):
        return (0, jnp.where(r == q, n, jnp.where(r < q, 0, n_tiles - 1)))

    return pl.pallas_call(
        functools.partial(gather_body, n_src, scaled),
        grid=(n_src, n_tiles),
        in_specs=[pl.BlockSpec(memory_space=pltpu.SMEM)] + [pl.BlockSpec(t.shape, lambda r, n: (0, 0)) for t in routes]
        + [pl.BlockSpec((tokens, tile), functools.partial(src_map, q)) for q in range(n_src)],
        out_specs=pl.BlockSpec((n_exp, cap, tile), lambda r, n: (0, r, n)),
        out_shape=jax.ShapeDtypeStruct((n_exp, n_src * cap, dim), BF16),
        scratch_shapes=[pltpu.VMEM((slots, tokens), BF16), pltpu.VMEM((slots, 1), F32)],
        compiler_params=params(2),
        cost_estimate=cost(2 * n_src * slots * tokens * dim, 2 * n_src * (tokens + slots) * dim),
        name="gather_rows",
    )(base, *routes, *sources)


def act_forward(rows, gate, up):
    pre_gate = dot_nt(rows, gate).astype(BF16)
    pre_up = dot_nt(rows, up).astype(BF16)
    gate_f = pre_gate.astype(F32)
    act_mix = (gate_f * jax.nn.sigmoid(gate_f) * pre_up.astype(F32)).astype(BF16)
    return pre_gate, pre_up, act_mix


def act_backward(d_mix, pre_gate, pre_up):
    d_mix = d_mix.astype(BF16).astype(F32)
    gate_f = pre_gate.astype(F32)
    sig = jax.nn.sigmoid(gate_f)
    d_gate = (d_mix * pre_up.astype(F32) * sig * (1.0 + gate_f * (1.0 - sig))).astype(BF16)
    d_up = (d_mix * gate_f * sig).astype(BF16)
    return d_gate, d_up


def store_halves(lo_ref, hi_ref, cols, value):
    half = lo_ref.shape[1]
    lo_ref[0, :, cols] = value[:half].astype(BF16)
    hi_ref[0, :, cols] = value[half:].astype(BF16)


def forward_body(tile, rows_ref, gate_ref, up_ref, *refs):
    a_ref, u_ref, m_ref = refs[-5:-2] if len(refs) == 6 else refs
    pre_gate, pre_up, act_mix = act_forward(rows_ref[0], gate_ref[0], up_ref[0])
    a_ref[0] = pre_gate
    u_ref[0] = pre_up
    m_ref[0] = act_mix
    if len(refs) == 6:
        down_ref, lo_ref, hi_ref = refs[0], refs[4], refs[5]
        for n in range(lo_ref.shape[-1] // tile):
            cols = pl.ds(n * tile, tile)
            store_halves(lo_ref, hi_ref, cols, dot_nn(act_mix, down_ref[0, :, cols]))


def backward_body(tile, rows_ref, a_ref, u_ref, down_ref, *refs):
    dg_ref, du_ref = refs[2:4] if len(refs) == 6 else refs
    d_gate, d_up = act_backward(dot_nt(rows_ref[0], down_ref[0]), a_ref[0], u_ref[0])
    dg_ref[0] = d_gate
    du_ref[0] = d_up
    if len(refs) == 6:
        gate_ref, up_ref, lo_ref, hi_ref = refs[0], refs[1], refs[4], refs[5]
        for n in range(lo_ref.shape[-1] // tile):
            cols = pl.ds(n * tile, tile)
            store_halves(lo_ref, hi_ref, cols, dot_nn(d_gate, gate_ref[0, :, cols]) + dot_nn(d_up, up_ref[0, :, cols]))


def expert_specs(rows, ff):
    n_exp, n_rows, dim = rows.shape
    w_spec = pl.BlockSpec((1, ff, dim), lambda e: (e, 0, 0))
    r_spec = pl.BlockSpec((1, n_rows, dim), lambda e: (e, 0, 0))
    f_spec = pl.BlockSpec((1, n_rows, ff), lambda e: (e, 0, 0))
    f_shape = jax.ShapeDtypeStruct((n_exp, n_rows, ff), BF16)
    h_spec = pl.BlockSpec((1, n_rows // 2, dim), lambda e: (e, 0, 0))
    h_shape = jax.ShapeDtypeStruct((n_exp, n_rows // 2, dim), BF16)
    return w_spec, r_spec, f_spec, f_shape, h_spec, h_shape


def expert_cost(rows, ff, dots):
    n_exp, n_rows, dim = rows.shape
    return cost(2 * dots * n_exp * n_rows * dim * ff, 2 * n_exp * (dots * ff * dim + 2 * n_rows * dim))


def expert_forward(rows, gate_t, up_t, down=None):
    ff = gate_t.shape[1]
    w_spec, r_spec, f_spec, f_shape, h_spec, h_shape = expert_specs(rows, ff)
    more = down is not None
    return pl.pallas_call(
        functools.partial(forward_body, 1024),
        grid=(rows.shape[0],),
        in_specs=[r_spec, w_spec, w_spec] + [w_spec] * more,
        out_specs=[f_spec] * 3 + [h_spec] * (2 * more),
        out_shape=[f_shape] * 3 + [h_shape] * (2 * more),
        compiler_params=params(1),
        cost_estimate=expert_cost(rows, ff, 2 + more),
        name="expert_forward",
    )(rows, gate_t, up_t, *((down,) if more else ()))


def expert_backward(rows, a, u, down, weights=()):
    ff = down.shape[1]
    w_spec, r_spec, f_spec, f_shape, h_spec, h_shape = expert_specs(rows, ff)
    more = len(weights)
    return pl.pallas_call(
        functools.partial(backward_body, 1024),
        grid=(rows.shape[0],),
        in_specs=[r_spec, f_spec, f_spec, w_spec] + [w_spec] * more,
        out_specs=[f_spec] * 2 + [h_spec] * more,
        out_shape=[f_shape] * 2 + [h_shape] * more,
        compiler_params=params(1),
        cost_estimate=expert_cost(rows, ff, 1 + more),
        name="expert_backward",
    )(rows, a, u, down, *weights)


def chunk_body(has_base, last, *refs):
    rows_ref, down_ref, refs = refs[0], refs[1], refs[2:]
    d_mix = dot_nt(rows_ref[0], down_ref[0])
    if has_base:
        d_mix = refs[0][0] + d_mix
        refs = refs[1:]
    if last:
        a_ref, u_ref, dg_ref, du_ref = refs
        dg_ref[0], du_ref[0] = act_backward(d_mix, a_ref[0], u_ref[0])
    else:
        refs[0][0] = d_mix


def backward_chunk(rows, start, down, base, acts=()):
    n_exp, n_rows, width = rows.shape
    ff = down.shape[1]
    w_spec = pl.BlockSpec((1, ff, width), lambda e: (e, 0, start // width))
    r_spec = pl.BlockSpec((1, n_rows, width), lambda e: (e, 0, 0))
    f_spec = pl.BlockSpec((1, n_rows, ff), lambda e: (e, 0, 0))
    sums = () if base is None else (base,)
    shape = jax.ShapeDtypeStruct((n_exp, n_rows, ff), BF16 if acts else F32)
    return pl.pallas_call(
        functools.partial(chunk_body, base is not None, bool(acts)),
        grid=(n_exp,),
        in_specs=[r_spec, w_spec] + [f_spec] * (len(sums) + len(acts)),
        out_specs=[f_spec] * 2 if acts else f_spec,
        out_shape=[shape] * 2 if acts else shape,
        compiler_params=params(1),
        cost_estimate=expert_cost(rows, ff, 1),
        name="backward_chunk",
    )(rows, down, *sums, *acts)


def wgrad_body(n_parts, adds, *refs):
    small, wide, base = refs[:n_parts], refs[n_parts:2 * n_parts], refs[2 * n_parts:-3]
    out_ref, small_all, wide_all = refs[-3:]
    if n_parts == 1:
        sums = dot_tn(small[0][0], wide[0][0])
    else:
        start = 0
        for part in range(n_parts):
            span = pl.ds(start, small[part].shape[1])
            start += small[part].shape[1]

            @pl.when(pl.program_id(1) == 0)
            def _():
                small_all[span, :] = small[part][0]

            wide_all[span, :] = wide[part][0]
        sums = dot_tn(small_all[...], wide_all[...])
    out_ref[0] = base[0][0] + sums if adds else sums


def weight_grad(small, wide, base=None, adds=False, start=0, width=None, tile=2048):
    n_exp, _, ff = small[0].shape
    dim = wide[0].shape[2]
    width = width or dim
    tile = min(tile, width)
    total = sum(s.shape[1] for s in small)
    skip = start // tile

    def wide_spec(w):
        first = skip if w.shape[2] == dim else 0
        return pl.BlockSpec((1, w.shape[1], tile), lambda e, n: (e, 0, n + first))

    out_spec = pl.BlockSpec((1, ff, tile), lambda e, n: (e, 0, n + skip))
    base_specs = [] if base is None else [out_spec if adds else pl.BlockSpec(memory_space=pl.ANY)]
    stacked = total if len(small) > 1 else 16
    return pl.pallas_call(
        functools.partial(wgrad_body, len(small), adds),
        grid=(n_exp, width // tile),
        in_specs=[pl.BlockSpec((1, s.shape[1], ff), lambda e, n: (e, 0, 0)) for s in small] + [wide_spec(w) for w in wide] + base_specs,
        out_specs=out_spec,
        out_shape=jax.ShapeDtypeStruct((n_exp, ff, dim), F32),
        input_output_aliases={} if base is None else {2 * len(small): 0},
        scratch_shapes=[pltpu.VMEM((stacked, ff), BF16), pltpu.VMEM((stacked, tile), BF16)],
        compiler_params=params(2),
        cost_estimate=cost(2 * n_exp * total * width * ff, n_exp * (4 * ff * width + 2 * total * (width + ff))),
        name="weight_grad",
    )(*small, *wide, *(() if base is None else (base,)))


def fill_hot(tgt_ref, first_slot, *hots):
    chunk = 128
    slots = hots[0].shape[1]

    @pl.loop(0, hots[0].shape[0] // chunk)
    def _(c):
        rows = pl.ds(pl.multiple_of(c * chunk, chunk), chunk)
        lanes = lax.broadcasted_iota(jnp.int32, (chunk, slots), 1) + first_slot
        first, second = tgt_ref[rows, 0:1] == lanes, tgt_ref[rows, 1:2] == lanes
        if len(hots) == 2:
            hots[0][rows, :] = first.astype(F32).astype(BF16)
            hots[1][rows, :] = second.astype(F32).astype(BF16)
        else:
            hots[0][rows, :] = (first | second).astype(F32).astype(BF16)


def stack_rows(rets, rows):
    n_exp, cap, tile = rets[0].shape
    for q, ret in enumerate(rets):
        rows[pl.ds(q * n_exp * cap, n_exp * cap), :] = ret[...].reshape(n_exp * cap, tile)
    return rows[...]


def combine_body(n_ret, first_slot, last, tgt_ref, p_ref, dout_ref, in_ref, *refs):
    rets, refs = refs[:n_ret], refs[n_ret:]
    if last:
        ids_ref, dgate_in, out_ref, dlog_ref, hot_a, hot_b, rows, dgate_ref = refs
    else:
        out_ref, dgate_ref, hot_a, hot_b, rows = refs

    @pl.when(pl.program_id(0) == 0)
    def _():
        fill_hot(tgt_ref, first_slot, hot_a, hot_b)
        dgate_ref[...] = dgate_in[...] if last else jnp.zeros_like(dgate_ref)

    stacked = stack_rows(rets, rows)
    first, second = dot_nn(hot_a[...], stacked), dot_nn(hot_b[...], stacked)
    dout = dout_ref[...].astype(F32)
    out_ref[...] = (in_ref[...].astype(F32) + (p_ref[:, 0:1] * first + p_ref[:, 1:2] * second)).astype(out_ref.dtype)
    dgate_ref[:, 0:1] += jnp.sum(first * dout, axis=1, keepdims=True)
    dgate_ref[:, 1:2] += jnp.sum(second * dout, axis=1, keepdims=True)

    if last:
        @pl.when(pl.program_id(0) == pl.num_programs(0) - 1)
        def _():
            p_a, p_b = p_ref[:, 0:1], p_ref[:, 1:2]
            g_a, g_b = dgate_ref[:, 0:1], dgate_ref[:, 1:2]
            mean = p_a * g_a + p_b * g_b
            expert = lax.broadcasted_iota(jnp.int32, dlog_ref.shape, 1)
            d_a = jnp.where(ids_ref[:, 0:1] == expert, p_a * (g_a - mean), 0.0)
            d_b = jnp.where(ids_ref[:, 1:2] == expert, p_b * (g_b - mean), 0.0)
            dlog_ref[...] = (d_a + d_b).astype(BF16)


def combine(tgt, gate_probs, dout, base, rets, first_slot, ids=None, dgates=None, experts=0, tile=512):
    tokens, dim = base.shape
    n_exp, cap, _ = rets[0].shape
    slots = len(rets) * n_exp * cap
    last = ids is not None
    full = pl.BlockSpec((tokens, 2), lambda n: (0, 0))
    cols = pl.BlockSpec((tokens, tile), lambda n: (0, n))
    ret_spec = pl.BlockSpec((n_exp, cap, tile), lambda n: (0, 0, n))
    side = pl.BlockSpec((tokens, experts), lambda n: (0, 0)) if last else full
    side_shape = jax.ShapeDtypeStruct((tokens, experts), BF16) if last else jax.ShapeDtypeStruct((tokens, 2), F32)
    return pl.pallas_call(
        functools.partial(combine_body, len(rets), first_slot, last),
        grid=(dim // tile,),
        in_specs=[full, full, cols, cols] + [ret_spec] * len(rets) + [full, full] * last,
        out_specs=[cols, side],
        out_shape=[jax.ShapeDtypeStruct((tokens, dim), BF16 if last else F32), side_shape],
        scratch_shapes=[pltpu.VMEM((tokens, slots), BF16), pltpu.VMEM((tokens, slots), BF16), pltpu.VMEM((slots, tile), BF16)] + [pltpu.VMEM((tokens, 2), F32)] * last,
        compiler_params=params(1),
        cost_estimate=cost(4 * tokens * slots * dim, 2 * (4 * tokens + slots) * dim),
        name="combine",
    )(tgt, gate_probs, dout, base, *rets, *((ids, dgates) if last else ()))


def near_body(n_ret, tgt_ref, *refs):
    rets, (out_ref, hot, rows) = refs[:n_ret], refs[n_ret:]

    @pl.when(pl.program_id(0) == 0)
    def _():
        fill_hot(tgt_ref, 0, hot)

    out_ref[...] = dot_nn(hot[...], stack_rows(rets, rows))


def near_rows(tgt, rets, tile=512):
    tokens = tgt.shape[0]
    n_exp, cap, dim = rets[0].shape
    slots = len(rets) * n_exp * cap
    return pl.pallas_call(
        functools.partial(near_body, len(rets)),
        grid=(dim // tile,),
        in_specs=[pl.BlockSpec((tokens, 2), lambda n: (0, 0))] + [pl.BlockSpec((n_exp, cap, tile), lambda n: (0, 0, n))] * len(rets),
        out_specs=pl.BlockSpec((tokens, tile), lambda n: (0, n)),
        out_shape=jax.ShapeDtypeStruct((tokens, dim), F32),
        scratch_shapes=[pltpu.VMEM((tokens, slots), BF16), pltpu.VMEM((slots, tile), BF16)],
        compiler_params=params(1),
        cost_estimate=cost(2 * tokens * slots * dim, 2 * (2 * tokens + slots) * dim),
        name="near_rows",
    )(tgt, *rets)


def finish_body(n_ret, first_slot, tgt_ref, dlog_ref, stat_ref, router_ref, gain_ref, x_ref, dout_ref, near_ref, *refs):
    rets = refs[:n_ret]
    gx_ref, ggain_ref, gbias_ref, hot, rows, d_hid, row_sums = refs[n_ret:]
    phase, n = pl.program_id(0), pl.program_id(1)
    tile = rets[0].shape[2]
    dim = d_hid.shape[1]
    cols = pl.ds(pl.multiple_of(n * tile, tile), tile)

    @pl.when((phase == 0) & (n == 0))
    def _():
        fill_hot(tgt_ref, first_slot, hot)
        row_sums[...] = jnp.zeros_like(row_sums)

    inv_std = stat_ref[:, 1:2]
    normed = (x_ref[...].astype(F32) - stat_ref[:, 0:1]) * inv_std

    @pl.when(phase == 0)
    def _():
        far = dot_nn(hot[...], stack_rows(rets, rows))
        rounded = (near_ref[...] + far + dot_nn(dlog_ref[...], router_ref[...])).astype(BF16)
        d_hid[:, cols] = rounded
        d_h = rounded.astype(F32)
        weighted = d_h * normed
        ggain_ref[...] = jnp.sum(weighted, axis=0, keepdims=True)
        gbias_ref[...] = jnp.sum(d_h, axis=0, keepdims=True)
        row_sums[:, 0:1] += jnp.sum(d_h * gain_ref[...], axis=1, keepdims=True)
        row_sums[:, 1:2] += jnp.sum(weighted * gain_ref[...], axis=1, keepdims=True)

    @pl.when(phase == 1)
    def _():
        d_norm = d_hid[:, cols].astype(F32) * gain_ref[...]
        mean_dn = row_sums[:, 0:1] * (1.0 / dim)
        mean_dnn = row_sums[:, 1:2] * (1.0 / dim)
        gx_ref[...] = (dout_ref[...].astype(F32) + inv_std * (d_norm - mean_dn - normed * mean_dnn)).astype(BF16)


def finish(tgt, d_logits, stats, router_t, gain, x_loc, dout, near, rets, first_slot, tile=512):
    tokens, dim = x_loc.shape
    experts = d_logits.shape[1]
    n_exp, cap, _ = rets[0].shape
    slots = len(rets) * n_exp * cap
    last = dim // tile - 1

    def early(p, n):
        return jnp.where(p == 0, n, last)

    full = pl.BlockSpec((tokens, 2), lambda p, n: (0, 0))
    both = pl.BlockSpec((tokens, tile), lambda p, n: (0, n))
    late = pl.BlockSpec((tokens, tile), lambda p, n: (0, n * p))
    line = pl.BlockSpec((1, tile), lambda p, n: (0, n))
    early_line = pl.BlockSpec((1, tile), lambda p, n: (0, early(p, n)))
    ret_spec = pl.BlockSpec((n_exp, cap, tile), lambda p, n: (0, 0, early(p, n)))
    return pl.pallas_call(
        functools.partial(finish_body, len(rets), first_slot),
        grid=(2, dim // tile),
        in_specs=[full, pl.BlockSpec((tokens, experts), lambda p, n: (0, 0)), full, pl.BlockSpec((experts, tile), lambda p, n: (0, n)), line, both, late]
        + [pl.BlockSpec((tokens, tile), lambda p, n: (0, early(p, n)))] + [ret_spec] * len(rets),
        out_specs=[late, early_line, early_line],
        out_shape=[jax.ShapeDtypeStruct((tokens, dim), BF16), jax.ShapeDtypeStruct((1, dim), F32), jax.ShapeDtypeStruct((1, dim), F32)],
        scratch_shapes=[pltpu.VMEM((tokens, slots), BF16), pltpu.VMEM((slots, tile), BF16), pltpu.VMEM((tokens, dim), BF16), pltpu.VMEM((tokens, 2), F32)],
        compiler_params=params(2),
        cost_estimate=cost(2 * tokens * slots * dim, 2 * (7 * tokens + slots) * dim),
        name="finish",
    )(tgt, d_logits, stats, router_t, gain, x_loc, dout, near, *rets)


def solution(mesh):
    n_dp, n_ep = mesh.shape["dp"], mesh.shape["ep"]
    tok_spec = P(("dp", "ep"), None)
    exp_spec = P("ep", None, None)

    def swap(value, bits):
        return lax.ppermute(value, "ep", [(j, j ^ bits) for j in range(n_ep)])

    def cross(value):
        return lax.ppermute(value, "dp", [(i, i ^ 1) for i in range(n_dp)])

    def total(value):
        value = value + swap(value, 1)
        value = value + cross(value)
        return value + swap(value, 2)

    def local_step(x_loc, ln_gain, ln_bias, w_router, w_gate, w_up, w_down, ids_loc, slots_loc, dout):
        tokens, dim = x_loc.shape
        experts = w_router.shape[1]
        n_exp = w_gate.shape[0]
        cap = capacity_for(tokens, experts, ids_loc.shape[1])
        local = n_exp * cap
        j = lax.axis_index("ep")
        gate_t, up_t = jnp.swapaxes(w_gate, 1, 2), jnp.swapaxes(w_up, 1, 2)
        base = (j * local).astype(jnp.int32)[None]

        def gather(routes, sources, scaled):
            return gather_rows(base, routes, sources, n_exp, cap, scaled)

        hidden, stats, logits = norm_router(x_loc, ln_gain[None], ln_bias[None], w_router.T)
        h_x, h_c, g_0 = swap(hidden, 2), swap(hidden, 1), cross(hidden)

        ids_t, slots_t, logits_t = ids_loc.T, slots_loc.T, logits.T
        kept = slots_t >= 0
        target = jnp.where(kept, ids_t * cap + slots_t, -1)
        picked = jnp.sum(jnp.where(ids_t[:, None, :] == jnp.arange(experts)[None, :, None], logits_t[None], 0.0), axis=1)
        probs = jax.nn.softmax(picked, axis=0)
        route = jnp.concatenate([target.astype(F32), probs, jnp.zeros((4, tokens), F32)])
        r_x, r_c, r_0 = swap(route, 2), swap(route, 1), cross(route)
        d_x, d_c, e_0 = swap(dout, 2), swap(dout, 1), cross(dout)

        rows_a = gather((route, r_c), (hidden, h_c), False)
        act_a = expert_forward(rows_a, gate_t, up_t, w_down)
        grads_a = gather((route, r_c), (dout, d_c), True)
        back_a = expert_backward(grads_a, act_a[0], act_a[1], w_down, (gate_t, up_t))
        y_c = swap(act_a[4], 1)
        d_rows_c = swap(back_a[3], 1)
        tgt = jnp.where(kept, (ids_t // n_exp ^ j) * local + (ids_t % n_exp) * cap + slots_t, -1).T
        p_cols = probs.T
        moe_near, dgate_near = combine(tgt, p_cols, dout, x_loc, (act_a[3], y_c), 0)
        d_near = near_rows(tgt, (back_a[2], d_rows_c))

        h_xc, r_xc = swap(h_x, 1), swap(r_x, 1)
        g_2, r_2 = cross(h_x), cross(r_x)
        rows_b = gather((r_x, r_xc), (h_x, h_xc), False)
        act_b = expert_forward(rows_b, gate_t, up_t, w_down)
        y_home = (swap(act_b[3], 2), swap(act_b[4], 3))

        g_1, r_1 = swap(g_0, 1), swap(r_0, 1)
        rows_o = gather((r_0, r_1), (g_0, g_1), False)
        act_o = expert_forward(rows_o, gate_t, up_t)

        d_xc = swap(d_x, 1)
        grads_b = gather((r_x, r_xc), (d_x, d_xc), True)
        back_b = expert_backward(grads_b, act_b[0], act_b[1], w_down, (gate_t, up_t))
        d_home = (swap(back_b[2], 2), swap(back_b[3], 3))
        chunks = [(dim // 4 * s, dim // 4 * w) for s, w in ((0, 2), (2, 1), (3, 1))]
        e_2 = [cross(lax.slice_in_dim(d_x, s, s + w, axis=1)) for s, w in chunks]

        e_1 = swap(e_0, 1)
        grads_o = gather((r_0, r_1), (e_0, e_1), True)
        back_o = expert_backward(grads_o, act_o[0], act_o[1], w_down)
        grad_gate = weight_grad((back_a[0], back_b[0], back_o[0]), (rows_a, rows_b, rows_o))
        grad_up = weight_grad((back_a[1], back_b[1], back_o[1]), (rows_a, rows_b, rows_o))

        g_3, r_3 = swap(g_2, 1), swap(r_2, 1)
        rows_q = gather((r_2, r_3), (g_2, g_3), False)
        act_q = expert_forward(rows_q, gate_t, up_t)

        moe_out, d_logits = combine(tgt, p_cols, dout, moe_near, y_home, 2 * local, ids_loc, dgate_near, experts)
        grad_router = total(jnp.einsum("te,tm->em", d_logits, hidden, preferred_element_type=F32))

        grad_down, d_mix = None, None
        for c, (start, width) in enumerate(chunks):
            e_3 = swap(e_2[c], 1)
            grads_q = gather((r_2, r_3), (e_2[c], e_3), True)
            last = c == len(chunks) - 1
            d_mix = backward_chunk(grads_q, start, w_down, d_mix, act_q[:2] if last else ())
            grad_down = weight_grad((act_a[2], act_b[2], act_o[2], act_q[2]), (grads_a, grads_b, grads_o, grads_q), grad_down, False, start, width)
        grad_gate = weight_grad((d_mix[0],), (rows_q,), grad_gate, True)
        grad_up = weight_grad((d_mix[1],), (rows_q,), grad_up, True)

        grad_x, g_gain, g_bias = finish(tgt, d_logits, stats, w_router.T, ln_gain[None], x_loc, dout, d_near, d_home, 2 * local)
        g_norm = total(jnp.concatenate([g_gain, g_bias]))
        return (moe_out, grad_x, g_norm[0], g_norm[1], grad_router.T, jnp.swapaxes(grad_gate, 1, 2), jnp.swapaxes(grad_up, 1, 2), grad_down)

    return jax.shard_map(local_step, mesh=mesh, in_specs=(tok_spec, P(None), P(None), P(None, None), exp_spec, exp_spec, exp_spec, tok_spec, tok_spec, tok_spec), out_specs=(tok_spec, tok_spec, P(None), P(None), P(None, None), exp_spec, exp_spec, exp_spec), check_vma=False)
```

```python
import functools

import jax
import jax.numpy as jnp
from jax import lax
from jax.experimental import pallas as pl
from jax.experimental.pallas import tpu as pltpu
from jax.sharding import PartitionSpec as P


LN_EPS = 1e-5
F32 = jnp.float32
BF16 = jnp.bfloat16
VMEM_LIMIT = 62 * 1024 * 1024


def capacity_for(tokens_dev, experts, n_top):
    return 8 * ((5 * tokens_dev * n_top + 32 * experts - 1) // (32 * experts))


def params(n_axes):
    return pltpu.CompilerParams(dimension_semantics=("arbitrary",) * n_axes, vmem_limit_bytes=VMEM_LIMIT)


def cost(flops, nbytes):
    return pl.CostEstimate(flops=int(flops), bytes_accessed=int(nbytes), transcendentals=0)


def dot(lhs, rhs, l_dim, r_dim):
    return lax.dot_general(lhs, rhs, (((l_dim,), (r_dim,)), ((), ())), preferred_element_type=F32)


def dot_nn(lhs, rhs):
    return dot(lhs, rhs, 1, 0)


def dot_nt(lhs, rhs):
    return dot(lhs, rhs, 1, 1)


def dot_tn(lhs, rhs):
    return dot(lhs, rhs, 0, 0)


def col(ref, k):
    return ref[:, k:k + 1]


def whole(*shape):
    return pl.BlockSpec(shape, lambda *_: (0,) * len(shape))


def leading(*shape):
    return pl.BlockSpec((1,) + shape, lambda e, *_: (e, 0, 0))


def striped(*shape):
    return pl.BlockSpec(shape, lambda n: (0,) * (len(shape) - 1) + (n,))


def norm_body(x_ref, gain_ref, bias_ref, router_ref, hid_ref, stat_ref, logit_ref):
    x_f = x_ref[...].astype(F32)
    mean = jnp.mean(x_f, axis=-1, keepdims=True)
    centered = x_f - mean
    inv_std = lax.rsqrt(jnp.mean(centered * centered, axis=-1, keepdims=True) + LN_EPS)
    hidden = (centered * inv_std * gain_ref[...] + bias_ref[...]).astype(BF16)
    hid_ref[...] = hidden
    stat_ref[...] = jnp.concatenate([mean, inv_std], axis=1)
    logit_ref[...] = dot_nt(hidden, router_ref[...])


def norm_router(x_loc, gain, bias, router_t, tile=256):
    tokens, dim = x_loc.shape
    experts = router_t.shape[0]
    line = whole(1, dim)

    def by_row(width):
        return pl.BlockSpec((tile, width), lambda t: (t, 0))

    return pl.pallas_call(
        norm_body,
        grid=(tokens // tile,),
        in_specs=[by_row(dim), line, line, whole(experts, dim)],
        out_specs=[by_row(dim), by_row(2), by_row(experts)],
        out_shape=[jax.ShapeDtypeStruct((tokens, dim), BF16), jax.ShapeDtypeStruct((tokens, 2), F32), jax.ShapeDtypeStruct((tokens, experts), F32)],
        compiler_params=params(1),
        cost_estimate=cost(20 * tokens * dim, 4 * tokens * dim),
        name="norm_router",
    )(x_loc, gain, bias, router_t)


def gather_body(n_src, first_use, *refs):
    if first_use:
        base_ref, routes, srcs, (out_ref, hot_ref, p_ref) = refs[0], refs[1:n_src + 1], refs[n_src + 1:-3], refs[-3:]
    else:
        hot_ref, p_ref, srcs, out_ref = refs[0], refs[1], refs[2:-1], refs[-1]
    r, n = pl.program_id(0), pl.program_id(1)
    n_exp, cap, _ = out_ref.shape
    tokens = hot_ref.shape[2]

    for q in range(n_src):
        if first_use:
            @pl.when((r == q) & (n == 0))
            def _():
                id_a, id_b, p_a, p_b = (routes[q][k:k + 1, :] for k in range(4))
                for e in range(n_exp):
                    span = pl.ds(e * cap, cap)
                    slot = (lax.broadcasted_iota(jnp.int32, (cap, tokens), 0) + (base_ref[0] + e * cap)).astype(F32)
                    first, second = id_a == slot, id_b == slot
                    hot_ref[0, span, :] = (first | second).astype(F32).astype(BF16)
                    p_ref[0, span, :] = jnp.sum(jnp.where(first, p_a, jnp.where(second, p_b, 0.0)), axis=1, keepdims=True)

        @pl.when(r == q)
        def _():
            rows = dot_nn(hot_ref[0], srcs[q][...])
            if not first_use:
                rows = rows * p_ref[0]
            out_ref[...] = rows.astype(BF16).reshape(out_ref.shape)


def gather_call(first_use, sources, n_exp, cap, args, tile=2048):
    n_src = len(sources)
    tokens, dim = sources[0].shape
    tile = min(tile, dim)
    slots = n_exp * cap
    last = dim // tile - 1

    def src_map(q, r, n):
        return (0, jnp.where(r == q, n, jnp.where(r < q, 0, last)))

    hot_specs = [leading(slots, tokens), leading(slots, 1)]
    hot_shapes = [jax.ShapeDtypeStruct((n_src, slots, tokens), BF16), jax.ShapeDtypeStruct((n_src, slots, 1), F32)]
    arg_specs = [pl.BlockSpec(memory_space=pltpu.SMEM)] + [whole(*t.shape) for t in args[1:]] if first_use else hot_specs
    out_spec = pl.BlockSpec((n_exp, cap, tile), lambda r, n: (0, r, n))
    out_shape = jax.ShapeDtypeStruct((n_exp, n_src * cap, dim), BF16)
    return pl.pallas_call(
        functools.partial(gather_body, n_src, first_use),
        grid=(n_src, dim // tile),
        in_specs=arg_specs + [pl.BlockSpec((tokens, tile), functools.partial(src_map, q)) for q in range(n_src)],
        out_specs=[out_spec] + hot_specs if first_use else out_spec,
        out_shape=[out_shape] + hot_shapes if first_use else out_shape,
        compiler_params=params(2),
        cost_estimate=cost(2 * n_src * slots * tokens * dim, 2 * n_src * (tokens + slots) * dim),
        name="gather_rows",
    )(*args, *sources)


def act_forward(rows, gate, up):
    pre_gate = dot_nt(rows, gate).astype(BF16)
    pre_up = dot_nt(rows, up).astype(BF16)
    gate_f = pre_gate.astype(F32)
    act_mix = (gate_f * jax.nn.sigmoid(gate_f) * pre_up.astype(F32)).astype(BF16)
    return pre_gate, pre_up, act_mix


def act_backward(d_mix, pre_gate, pre_up):
    d_mix = d_mix.astype(BF16).astype(F32)
    gate_f = pre_gate.astype(F32)
    sig = jax.nn.sigmoid(gate_f)
    d_gate = (d_mix * pre_up.astype(F32) * sig * (1.0 + gate_f * (1.0 - sig))).astype(BF16)
    d_up = (d_mix * gate_f * sig).astype(BF16)
    return d_gate, d_up


def store_halves(lo_ref, hi_ref, cols, value):
    half = lo_ref.shape[1]
    lo_ref[0, :, cols] = value[:half].astype(BF16)
    hi_ref[0, :, cols] = value[half:].astype(BF16)


def forward_body(tile, rows_ref, gate_ref, up_ref, *refs):
    a_ref, u_ref, m_ref = refs[-5:-2] if len(refs) == 6 else refs
    pre_gate, pre_up, act_mix = act_forward(rows_ref[0], gate_ref[0], up_ref[0])
    a_ref[0] = pre_gate
    u_ref[0] = pre_up
    m_ref[0] = act_mix
    if len(refs) == 6:
        down_ref, lo_ref, hi_ref = refs[0], refs[4], refs[5]
        for n in range(lo_ref.shape[-1] // tile):
            cols = pl.ds(n * tile, tile)
            store_halves(lo_ref, hi_ref, cols, dot_nn(act_mix, down_ref[0, :, cols]))


def backward_body(tile, rows_ref, a_ref, u_ref, down_ref, *refs):
    dg_ref, du_ref = refs[2:4] if len(refs) == 6 else refs
    d_gate, d_up = act_backward(dot_nt(rows_ref[0], down_ref[0]), a_ref[0], u_ref[0])
    dg_ref[0] = d_gate
    du_ref[0] = d_up
    if len(refs) == 6:
        gate_ref, up_ref, lo_ref, hi_ref = refs[0], refs[1], refs[4], refs[5]
        for n in range(lo_ref.shape[-1] // tile):
            cols = pl.ds(n * tile, tile)
            store_halves(lo_ref, hi_ref, cols, dot_nn(d_gate, gate_ref[0, :, cols]) + dot_nn(d_up, up_ref[0, :, cols]))


def expert_specs(rows, ff):
    n_exp, n_rows, dim = rows.shape
    w_spec, r_spec, f_spec, h_spec = leading(ff, dim), leading(n_rows, dim), leading(n_rows, ff), leading(n_rows // 2, dim)
    f_shape = jax.ShapeDtypeStruct((n_exp, n_rows, ff), BF16)
    h_shape = jax.ShapeDtypeStruct((n_exp, n_rows // 2, dim), BF16)
    return w_spec, r_spec, f_spec, f_shape, h_spec, h_shape


def expert_cost(rows, ff, dots):
    n_exp, n_rows, dim = rows.shape
    return cost(2 * dots * n_exp * n_rows * dim * ff, 2 * n_exp * (dots * ff * dim + 2 * n_rows * dim))


def expert_forward(rows, gate_t, up_t, down=None):
    ff = gate_t.shape[1]
    w_spec, r_spec, f_spec, f_shape, h_spec, h_shape = expert_specs(rows, ff)
    more = down is not None
    return pl.pallas_call(
        functools.partial(forward_body, 1024),
        grid=(rows.shape[0],),
        in_specs=[r_spec, w_spec, w_spec] + [w_spec] * more,
        out_specs=[f_spec] * 3 + [h_spec] * (2 * more),
        out_shape=[f_shape] * 3 + [h_shape] * (2 * more),
        compiler_params=params(1),
        cost_estimate=expert_cost(rows, ff, 2 + more),
        name="expert_forward",
    )(rows, gate_t, up_t, *((down,) if more else ()))


def expert_backward(rows, a, u, down, weights=()):
    ff = down.shape[1]
    w_spec, r_spec, f_spec, f_shape, h_spec, h_shape = expert_specs(rows, ff)
    more = len(weights)
    return pl.pallas_call(
        functools.partial(backward_body, 1024),
        grid=(rows.shape[0],),
        in_specs=[r_spec, f_spec, f_spec, w_spec] + [w_spec] * more,
        out_specs=[f_spec] * 2 + [h_spec] * more,
        out_shape=[f_shape] * 2 + [h_shape] * more,
        compiler_params=params(1),
        cost_estimate=expert_cost(rows, ff, 1 + more),
        name="expert_backward",
    )(rows, a, u, down, *weights)


def chunk_body(has_base, last, *refs):
    rows_ref, down_ref, refs = refs[0], refs[1], refs[2:]
    d_mix = dot_nt(rows_ref[0], down_ref[0])
    if has_base:
        d_mix = refs[0][0] + d_mix
        refs = refs[1:]
    if last:
        a_ref, u_ref, dg_ref, du_ref = refs
        dg_ref[0], du_ref[0] = act_backward(d_mix, a_ref[0], u_ref[0])
    else:
        refs[0][0] = d_mix


def backward_chunk(rows, start, down, base, acts=()):
    n_exp, n_rows, width = rows.shape
    ff = down.shape[1]
    w_spec = pl.BlockSpec((1, ff, width), lambda e: (e, 0, start // width))
    r_spec, f_spec = leading(n_rows, width), leading(n_rows, ff)
    sums = () if base is None else (base,)
    shape = jax.ShapeDtypeStruct((n_exp, n_rows, ff), BF16 if acts else F32)
    return pl.pallas_call(
        functools.partial(chunk_body, base is not None, bool(acts)),
        grid=(n_exp,),
        in_specs=[r_spec, w_spec] + [f_spec] * (len(sums) + len(acts)),
        out_specs=[f_spec] * 2 if acts else f_spec,
        out_shape=[shape] * 2 if acts else shape,
        compiler_params=params(1),
        cost_estimate=expert_cost(rows, ff, 1),
        name="backward_chunk",
    )(rows, down, *sums, *acts)


def wgrad_body(n_parts, adds, *refs):
    small, wide, base = refs[:n_parts], refs[n_parts:2 * n_parts], refs[2 * n_parts:-3]
    out_ref, small_all, wide_all = refs[-3:]
    if n_parts == 1:
        sums = dot_tn(small[0][0], wide[0][0])
    else:
        start = 0
        for part in range(n_parts):
            span = pl.ds(start, small[part].shape[1])
            start += small[part].shape[1]

            @pl.when(pl.program_id(1) == 0)
            def _():
                small_all[span, :] = small[part][0]

            wide_all[span, :] = wide[part][0]
        sums = dot_tn(small_all[...], wide_all[...])
    out_ref[0] = base[0][0] + sums if adds else sums


def weight_grad(small, wide, base=None, adds=False, start=0, width=None, tile=2048):
    n_exp, _, ff = small[0].shape
    dim = wide[0].shape[2]
    width = width or dim
    tile = min(tile, width)
    total = sum(s.shape[1] for s in small)
    skip = start // tile

    def wide_spec(w):
        first = skip if w.shape[2] == dim else 0
        return pl.BlockSpec((1, w.shape[1], tile), lambda e, n: (e, 0, n + first))

    out_spec = pl.BlockSpec((1, ff, tile), lambda e, n: (e, 0, n + skip))
    base_specs = [] if base is None else [out_spec if adds else pl.BlockSpec(memory_space=pl.ANY)]
    stacked = total if len(small) > 1 else 16
    return pl.pallas_call(
        functools.partial(wgrad_body, len(small), adds),
        grid=(n_exp, width // tile),
        in_specs=[leading(s.shape[1], ff) for s in small] + [wide_spec(w) for w in wide] + base_specs,
        out_specs=out_spec,
        out_shape=jax.ShapeDtypeStruct((n_exp, ff, dim), F32),
        input_output_aliases={} if base is None else {2 * len(small): 0},
        scratch_shapes=[pltpu.VMEM((stacked, ff), BF16), pltpu.VMEM((stacked, tile), BF16)],
        compiler_params=params(2),
        cost_estimate=cost(2 * n_exp * total * width * ff, n_exp * (4 * ff * width + 2 * total * (width + ff))),
        name="weight_grad",
    )(*small, *wide, *(() if base is None else (base,)))


def fill_hot(tgt_ref, first_slot, *hots):
    chunk = 128
    slots = hots[0].shape[1]

    @pl.loop(0, hots[0].shape[0] // chunk)
    def _(c):
        rows = pl.ds(pl.multiple_of(c * chunk, chunk), chunk)
        lanes = lax.broadcasted_iota(jnp.int32, (chunk, slots), 1) + first_slot
        first, second = (col(tgt_ref[rows, :], k) == lanes for k in range(2))
        if len(hots) == 2:
            hots[0][rows, :] = first.astype(F32).astype(BF16)
            hots[1][rows, :] = second.astype(F32).astype(BF16)
        else:
            hots[0][rows, :] = (first | second).astype(F32).astype(BF16)


def stack_rows(rets, rows):
    n_exp, cap, tile = rets[0].shape
    for q, ret in enumerate(rets):
        rows[pl.ds(q * n_exp * cap, n_exp * cap), :] = ret[...].reshape(n_exp * cap, tile)
    return rows[...]


def combine_body(n_ret, first_slot, last, tgt_ref, p_ref, dout_ref, in_ref, *refs):
    rets, refs = refs[:n_ret], refs[n_ret:]
    if last:
        ids_ref, dgate_in, out_ref, dlog_ref, hot_a, hot_b, rows, dgate_ref = refs
    else:
        out_ref, dgate_ref, hot_a, hot_b, rows = refs

    @pl.when(pl.program_id(0) == 0)
    def _():
        fill_hot(tgt_ref, first_slot, hot_a, hot_b)
        dgate_ref[...] = dgate_in[...] if last else jnp.zeros_like(dgate_ref)

    stacked = stack_rows(rets, rows)
    first, second = dot_nn(hot_a[...], stacked), dot_nn(hot_b[...], stacked)
    dout = dout_ref[...].astype(F32)
    out_ref[...] = (in_ref[...].astype(F32) + (col(p_ref, 0) * first + col(p_ref, 1) * second)).astype(out_ref.dtype)
    for k, rows_k in enumerate((first, second)):
        dgate_ref[:, k:k + 1] += jnp.sum(rows_k * dout, axis=1, keepdims=True)

    if last:
        @pl.when(pl.program_id(0) == pl.num_programs(0) - 1)
        def _():
            p_a, p_b = col(p_ref, 0), col(p_ref, 1)
            g_a, g_b = col(dgate_ref, 0), col(dgate_ref, 1)
            mean = p_a * g_a + p_b * g_b
            expert = lax.broadcasted_iota(jnp.int32, dlog_ref.shape, 1)
            d_a = jnp.where(col(ids_ref, 0) == expert, p_a * (g_a - mean), 0.0)
            d_b = jnp.where(col(ids_ref, 1) == expert, p_b * (g_b - mean), 0.0)
            dlog_ref[...] = (d_a + d_b).astype(BF16)


def combine(tgt, gate_probs, dout, base, rets, first_slot, ids=None, dgates=None, experts=0, tile=512):
    tokens, dim = base.shape
    n_exp, cap, _ = rets[0].shape
    slots = len(rets) * n_exp * cap
    last = ids is not None
    full, cols, ret_spec = whole(tokens, 2), striped(tokens, tile), striped(n_exp, cap, tile)
    side = whole(tokens, experts) if last else full
    side_shape = jax.ShapeDtypeStruct((tokens, experts), BF16) if last else jax.ShapeDtypeStruct((tokens, 2), F32)
    return pl.pallas_call(
        functools.partial(combine_body, len(rets), first_slot, last),
        grid=(dim // tile,),
        in_specs=[full, full, cols, cols] + [ret_spec] * len(rets) + [full, full] * last,
        out_specs=[cols, side],
        out_shape=[jax.ShapeDtypeStruct((tokens, dim), BF16 if last else F32), side_shape],
        scratch_shapes=[pltpu.VMEM((tokens, slots), BF16), pltpu.VMEM((tokens, slots), BF16), pltpu.VMEM((slots, tile), BF16)] + [pltpu.VMEM((tokens, 2), F32)] * last,
        compiler_params=params(1),
        cost_estimate=cost(4 * tokens * slots * dim, 2 * (4 * tokens + slots) * dim),
        name="combine",
    )(tgt, gate_probs, dout, base, *rets, *((ids, dgates) if last else ()))


def near_body(n_ret, tgt_ref, *refs):
    rets, (out_ref, hot, rows) = refs[:n_ret], refs[n_ret:]

    @pl.when(pl.program_id(0) == 0)
    def _():
        fill_hot(tgt_ref, 0, hot)

    out_ref[...] = dot_nn(hot[...], stack_rows(rets, rows))


def near_rows(tgt, rets, tile=512):
    tokens = tgt.shape[0]
    n_exp, cap, dim = rets[0].shape
    slots = len(rets) * n_exp * cap
    return pl.pallas_call(
        functools.partial(near_body, len(rets)),
        grid=(dim // tile,),
        in_specs=[whole(tokens, 2)] + [striped(n_exp, cap, tile)] * len(rets),
        out_specs=striped(tokens, tile),
        out_shape=jax.ShapeDtypeStruct((tokens, dim), F32),
        scratch_shapes=[pltpu.VMEM((tokens, slots), BF16), pltpu.VMEM((slots, tile), BF16)],
        compiler_params=params(1),
        cost_estimate=cost(2 * tokens * slots * dim, 2 * (2 * tokens + slots) * dim),
        name="near_rows",
    )(tgt, *rets)


def finish_body(n_ret, first_slot, tgt_ref, dlog_ref, stat_ref, router_ref, gain_ref, x_ref, dout_ref, near_ref, *refs):
    rets = refs[:n_ret]
    gx_ref, ggain_ref, gbias_ref, hot, rows, d_hid, row_sums = refs[n_ret:]
    phase, n = pl.program_id(0), pl.program_id(1)
    tile = rets[0].shape[2]
    dim = d_hid.shape[1]
    cols = pl.ds(pl.multiple_of(n * tile, tile), tile)

    @pl.when((phase == 0) & (n == 0))
    def _():
        fill_hot(tgt_ref, first_slot, hot)
        row_sums[...] = jnp.zeros_like(row_sums)

    inv_std = col(stat_ref, 1)
    normed = (x_ref[...].astype(F32) - col(stat_ref, 0)) * inv_std

    @pl.when(phase == 0)
    def _():
        far = dot_nn(hot[...], stack_rows(rets, rows))
        rounded = (near_ref[...] + far + dot_nn(dlog_ref[...], router_ref[...])).astype(BF16)
        d_hid[:, cols] = rounded
        d_h = rounded.astype(F32)
        weighted = d_h * normed
        ggain_ref[...] = jnp.sum(weighted, axis=0, keepdims=True)
        gbias_ref[...] = jnp.sum(d_h, axis=0, keepdims=True)
        for k, rows_k in enumerate((d_h, weighted)):
            row_sums[:, k:k + 1] += jnp.sum(rows_k * gain_ref[...], axis=1, keepdims=True)

    @pl.when(phase == 1)
    def _():
        d_norm = d_hid[:, cols].astype(F32) * gain_ref[...]
        mean_dn, mean_dnn = (col(row_sums, k) * (1.0 / dim) for k in range(2))
        gx_ref[...] = (dout_ref[...].astype(F32) + inv_std * (d_norm - mean_dn - normed * mean_dnn)).astype(BF16)


def finish(tgt, d_logits, stats, router_t, gain, x_loc, dout, near, rets, first_slot, tile=512):
    tokens, dim = x_loc.shape
    experts = d_logits.shape[1]
    n_exp, cap, _ = rets[0].shape
    slots = len(rets) * n_exp * cap
    last = dim // tile - 1

    def early(p, n):
        return jnp.where(p == 0, n, last)

    full = whole(tokens, 2)
    both = pl.BlockSpec((tokens, tile), lambda p, n: (0, n))
    late = pl.BlockSpec((tokens, tile), lambda p, n: (0, n * p))
    line = pl.BlockSpec((1, tile), lambda p, n: (0, n))
    early_line = pl.BlockSpec((1, tile), lambda p, n: (0, early(p, n)))
    ret_spec = pl.BlockSpec((n_exp, cap, tile), lambda p, n: (0, 0, early(p, n)))
    return pl.pallas_call(
        functools.partial(finish_body, len(rets), first_slot),
        grid=(2, dim // tile),
        in_specs=[full, whole(tokens, experts), full, pl.BlockSpec((experts, tile), lambda p, n: (0, n)), line, both, late]
        + [pl.BlockSpec((tokens, tile), lambda p, n: (0, early(p, n)))] + [ret_spec] * len(rets),
        out_specs=[late, early_line, early_line],
        out_shape=[jax.ShapeDtypeStruct((tokens, dim), BF16), jax.ShapeDtypeStruct((1, dim), F32), jax.ShapeDtypeStruct((1, dim), F32)],
        scratch_shapes=[pltpu.VMEM((tokens, slots), BF16), pltpu.VMEM((slots, tile), BF16), pltpu.VMEM((tokens, dim), BF16), pltpu.VMEM((tokens, 2), F32)],
        compiler_params=params(2),
        cost_estimate=cost(2 * tokens * slots * dim, 2 * (7 * tokens + slots) * dim),
        name="finish",
    )(tgt, d_logits, stats, router_t, gain, x_loc, dout, near, *rets)


def solution(mesh):
    n_dp, n_ep = mesh.shape["dp"], mesh.shape["ep"]
    tok_spec = P(("dp", "ep"), None)
    exp_spec = P("ep", None, None)

    def swap(value, bits):
        return lax.ppermute(value, "ep", [(j, j ^ bits) for j in range(n_ep)])

    def cross(value):
        return lax.ppermute(value, "dp", [(i, i ^ 1) for i in range(n_dp)])

    def total(value):
        value = value + swap(value, 1)
        value = value + cross(value)
        return value + swap(value, 2)

    def local_step(x_loc, ln_gain, ln_bias, w_router, w_gate, w_up, w_down, ids_loc, slots_loc, dout):
        tokens, dim = x_loc.shape
        experts = w_router.shape[1]
        n_exp = w_gate.shape[0]
        cap = capacity_for(tokens, experts, ids_loc.shape[1])
        local = n_exp * cap
        j = lax.axis_index("ep")
        gate_t, up_t = jnp.swapaxes(w_gate, 1, 2), jnp.swapaxes(w_up, 1, 2)
        base = (j * local).astype(jnp.int32)[None]

        def gather(routes, sources):
            rows, *hot = gather_call(True, sources, n_exp, cap, (base,) + routes)
            return rows, hot

        def gather_grads(hot, sources):
            return gather_call(False, sources, n_exp, cap, hot)

        hidden, stats, logits = norm_router(x_loc, ln_gain[None], ln_bias[None], w_router.T)
        h_x, h_c, g_0 = swap(hidden, 2), swap(hidden, 1), cross(hidden)

        ids_t, slots_t, logits_t = ids_loc.T, slots_loc.T, logits.T
        kept = slots_t >= 0
        target = jnp.where(kept, ids_t * cap + slots_t, -1)
        picked = jnp.sum(jnp.where(ids_t[:, None, :] == jnp.arange(experts)[None, :, None], logits_t[None], 0.0), axis=1)
        probs = jax.nn.softmax(picked, axis=0)
        route = jnp.concatenate([target.astype(F32), probs, jnp.zeros((4, tokens), F32)])
        r_x, r_c, r_0 = swap(route, 2), swap(route, 1), cross(route)
        d_x, d_c, e_0 = swap(dout, 2), swap(dout, 1), cross(dout)

        rows_a, hot_a = gather((route, r_c), (hidden, h_c))
        act_a = expert_forward(rows_a, gate_t, up_t, w_down)
        grads_a = gather_grads(hot_a, (dout, d_c))
        back_a = expert_backward(grads_a, act_a[0], act_a[1], w_down, (gate_t, up_t))
        y_c = swap(act_a[4], 1)
        d_rows_c = swap(back_a[3], 1)
        tgt = jnp.where(kept, (ids_t // n_exp ^ j) * local + (ids_t % n_exp) * cap + slots_t, -1).T
        p_cols = probs.T
        moe_near, dgate_near = combine(tgt, p_cols, dout, x_loc, (act_a[3], y_c), 0)
        d_near = near_rows(tgt, (back_a[2], d_rows_c))

        h_xc, r_xc = swap(h_x, 1), swap(r_x, 1)
        g_2, r_2 = cross(h_x), cross(r_x)
        rows_b, hot_b = gather((r_x, r_xc), (h_x, h_xc))
        act_b = expert_forward(rows_b, gate_t, up_t, w_down)
        y_home = (swap(act_b[3], 2), swap(act_b[4], 3))

        g_1, r_1 = swap(g_0, 1), swap(r_0, 1)
        rows_o, hot_o = gather((r_0, r_1), (g_0, g_1))
        act_o = expert_forward(rows_o, gate_t, up_t)

        d_xc = swap(d_x, 1)
        grads_b = gather_grads(hot_b, (d_x, d_xc))
        back_b = expert_backward(grads_b, act_b[0], act_b[1], w_down, (gate_t, up_t))
        d_home = (swap(back_b[2], 2), swap(back_b[3], 3))
        chunks = [(dim // 4 * s, dim // 4 * w) for s, w in ((0, 2), (2, 1), (3, 1))]
        e_2 = [cross(lax.slice_in_dim(d_x, s, s + w, axis=1)) for s, w in chunks]

        e_1 = swap(e_0, 1)
        grads_o = gather_grads(hot_o, (e_0, e_1))
        back_o = expert_backward(grads_o, act_o[0], act_o[1], w_down)
        grad_gate = weight_grad((back_a[0], back_b[0], back_o[0]), (rows_a, rows_b, rows_o))
        grad_up = weight_grad((back_a[1], back_b[1], back_o[1]), (rows_a, rows_b, rows_o))

        g_3, r_3 = swap(g_2, 1), swap(r_2, 1)
        rows_q, hot_q = gather((r_2, r_3), (g_2, g_3))
        act_q = expert_forward(rows_q, gate_t, up_t)

        moe_out, d_logits = combine(tgt, p_cols, dout, moe_near, y_home, 2 * local, ids_loc, dgate_near, experts)
        grad_router = total(jnp.einsum("te,tm->em", d_logits, hidden, preferred_element_type=F32))

        grad_down, d_mix = None, None
        for c, (start, width) in enumerate(chunks):
            e_3 = swap(e_2[c], 1)
            grads_q = gather_grads(hot_q, (e_2[c], e_3))
            last = c == len(chunks) - 1
            d_mix = backward_chunk(grads_q, start, w_down, d_mix, act_q[:2] if last else ())
            grad_down = weight_grad((act_a[2], act_b[2], act_o[2], act_q[2]), (grads_a, grads_b, grads_o, grads_q), grad_down, False, start, width)
        grad_gate = weight_grad((d_mix[0],), (rows_q,), grad_gate, True)
        grad_up = weight_grad((d_mix[1],), (rows_q,), grad_up, True)

        grad_x, g_gain, g_bias = finish(tgt, d_logits, stats, w_router.T, ln_gain[None], x_loc, dout, d_near, d_home, 2 * local)
        g_norm = total(jnp.concatenate([g_gain, g_bias]))
        return (moe_out, grad_x, g_norm[0], g_norm[1], grad_router.T, jnp.swapaxes(grad_gate, 1, 2), jnp.swapaxes(grad_up, 1, 2), grad_down)

    return jax.shard_map(local_step, mesh=mesh, in_specs=(tok_spec, P(None), P(None), P(None, None), exp_spec, exp_spec, exp_spec, tok_spec, tok_spec, tok_spec), out_specs=(tok_spec, tok_spec, P(None), P(None), P(None, None), exp_spec, exp_spec, exp_spec), check_vma=False)
```

```python
import functools

import jax
import jax.numpy as jnp
from jax import lax
from jax.experimental import pallas as pl
from jax.experimental.pallas import tpu as pltpu
from jax.sharding import PartitionSpec as P


LN_EPS = 1e-5
F32 = jnp.float32
BF16 = jnp.bfloat16
LANES = 128
VMEM_LIMIT = 62 * 1024 * 1024


def capacity_for(tokens_dev, experts, n_top):
    return 8 * ((5 * tokens_dev * n_top + 32 * experts - 1) // (32 * experts))


def params(n_axes):
    return pltpu.CompilerParams(dimension_semantics=("arbitrary",) * n_axes, vmem_limit_bytes=VMEM_LIMIT)


def cost(flops, nbytes):
    return pl.CostEstimate(flops=int(flops), bytes_accessed=int(nbytes), transcendentals=0)


def dot(lhs, rhs, l_dim, r_dim):
    return lax.dot_general(lhs, rhs, (((l_dim,), (r_dim,)), ((), ())), preferred_element_type=F32)


def dot_nn(lhs, rhs):
    return dot(lhs, rhs, 1, 0)


def dot_nt(lhs, rhs):
    return dot(lhs, rhs, 1, 1)


def dot_tn(lhs, rhs):
    return dot(lhs, rhs, 0, 0)


def col(ref, k):
    return ref[:, k:k + 1]


def fold_lanes(value):
    parts = [value[:, k:k + LANES] for k in range(0, value.shape[1], LANES)]
    return functools.reduce(jnp.add, parts)


def lane_total(ref, k):
    return jnp.sum(ref[:, k * LANES:(k + 1) * LANES], axis=1, keepdims=True)


def whole(*shape):
    return pl.BlockSpec(shape, lambda *_: (0,) * len(shape))


def leading(*shape):
    return pl.BlockSpec((1,) + shape, lambda e, *_: (e, 0, 0))


def striped(*shape):
    return pl.BlockSpec(shape, lambda n: (0,) * (len(shape) - 1) + (n,))


def norm_body(x_ref, gain_ref, bias_ref, router_ref, hid_ref, stat_ref, logit_ref):
    x_f = x_ref[...].astype(F32)
    mean = jnp.mean(x_f, axis=-1, keepdims=True)
    centered = x_f - mean
    inv_std = lax.rsqrt(jnp.mean(centered * centered, axis=-1, keepdims=True) + LN_EPS)
    hidden = (centered * inv_std * gain_ref[...] + bias_ref[...]).astype(BF16)
    hid_ref[...] = hidden
    stat_ref[...] = jnp.concatenate([mean, inv_std], axis=1)
    logit_ref[...] = dot_nt(hidden, router_ref[...])


def norm_router(x_loc, gain, bias, router_t, tile=256):
    tokens, dim = x_loc.shape
    experts = router_t.shape[0]
    line = whole(1, dim)

    def by_row(width):
        return pl.BlockSpec((tile, width), lambda t: (t, 0))

    return pl.pallas_call(
        norm_body,
        grid=(tokens // tile,),
        in_specs=[by_row(dim), line, line, whole(experts, dim)],
        out_specs=[by_row(dim), by_row(2), by_row(experts)],
        out_shape=[jax.ShapeDtypeStruct((tokens, dim), BF16), jax.ShapeDtypeStruct((tokens, 2), F32), jax.ShapeDtypeStruct((tokens, experts), F32)],
        compiler_params=params(1),
        cost_estimate=cost(20 * tokens * dim, 4 * tokens * dim),
        name="norm_router",
    )(x_loc, gain, bias, router_t)


def gather_body(n_src, first_use, scaled, *refs):
    if first_use:
        base_ref, routes, srcs, (out_ref, hot_ref, p_ref) = refs[0], refs[1:n_src + 1], refs[n_src + 1:-3], refs[-3:]
    else:
        hot_ref, p_ref, srcs, out_ref = refs[0], refs[1], refs[2:-1], refs[-1]
    r, n = pl.program_id(0), pl.program_id(1)
    n_exp, cap, _ = out_ref.shape
    tokens = hot_ref.shape[2]

    for q in range(n_src):
        if first_use:
            @pl.when((r == q) & (n == 0))
            def _():
                id_a, id_b, p_a, p_b = (routes[q][k:k + 1, :] for k in range(4))
                for e in range(n_exp):
                    span = pl.ds(e * cap, cap)
                    slot = (lax.broadcasted_iota(jnp.int32, (cap, tokens), 0) + (base_ref[0] + e * cap)).astype(F32)
                    first, second = id_a == slot, id_b == slot
                    hot_ref[0, span, :] = (first | second).astype(F32).astype(BF16)
                    p_ref[0, span, :] = jnp.sum(jnp.where(first, p_a, jnp.where(second, p_b, 0.0)), axis=1, keepdims=True)

        @pl.when(r == q)
        def _():
            rows = dot_nn(hot_ref[0], srcs[q][...])
            if scaled:
                rows = rows * p_ref[0]
            out_ref[...] = rows.astype(BF16).reshape(out_ref.shape)


def gather_call(first_use, scaled, sources, n_exp, cap, args, tile=2048):
    n_src = len(sources)
    tokens, dim = sources[0].shape
    tile = min(tile, dim)
    slots = n_exp * cap
    last = dim // tile - 1

    def src_map(q, r, n):
        return (0, jnp.where(r == q, n, jnp.where(r < q, 0, last)))

    hot_specs = [leading(slots, tokens), leading(slots, 1)]
    hot_shapes = [jax.ShapeDtypeStruct((n_src, slots, tokens), BF16), jax.ShapeDtypeStruct((n_src, slots, 1), F32)]
    arg_specs = [pl.BlockSpec(memory_space=pltpu.SMEM)] + [whole(*t.shape) for t in args[1:]] if first_use else hot_specs
    out_spec = pl.BlockSpec((n_exp, cap, tile), lambda r, n: (0, r, n))
    out_shape = jax.ShapeDtypeStruct((n_exp, n_src * cap, dim), BF16)
    return pl.pallas_call(
        functools.partial(gather_body, n_src, first_use, scaled),
        grid=(n_src, dim // tile),
        in_specs=arg_specs + [pl.BlockSpec((tokens, tile), functools.partial(src_map, q)) for q in range(n_src)],
        out_specs=[out_spec] + hot_specs if first_use else out_spec,
        out_shape=[out_shape] + hot_shapes if first_use else out_shape,
        compiler_params=params(2),
        cost_estimate=cost(2 * n_src * slots * tokens * dim, 2 * n_src * (tokens + slots) * dim),
        name="gather_rows",
    )(*args, *sources)


def act_forward(rows, gate, up):
    pre_gate = dot_nt(rows, gate).astype(BF16)
    pre_up = dot_nt(rows, up).astype(BF16)
    gate_f = pre_gate.astype(F32)
    act_mix = (gate_f * jax.nn.sigmoid(gate_f) * pre_up.astype(F32)).astype(BF16)
    return pre_gate, pre_up, act_mix


def act_backward(d_mix, pre_gate, pre_up):
    d_mix = d_mix.astype(BF16).astype(F32)
    gate_f = pre_gate.astype(F32)
    sig = jax.nn.sigmoid(gate_f)
    d_gate = (d_mix * pre_up.astype(F32) * sig * (1.0 + gate_f * (1.0 - sig))).astype(BF16)
    d_up = (d_mix * gate_f * sig).astype(BF16)
    return d_gate, d_up


def store_halves(lo_ref, hi_ref, cols, value):
    half = lo_ref.shape[1]
    lo_ref[0, :, cols] = value[:half].astype(BF16)
    hi_ref[0, :, cols] = value[half:].astype(BF16)


def forward_body(tile, rows_ref, gate_ref, up_ref, *refs):
    a_ref, u_ref, m_ref = refs[-5:-2] if len(refs) == 6 else refs
    pre_gate, pre_up, act_mix = act_forward(rows_ref[0], gate_ref[0], up_ref[0])
    a_ref[0] = pre_gate
    u_ref[0] = pre_up
    m_ref[0] = act_mix
    if len(refs) == 6:
        down_ref, lo_ref, hi_ref = refs[0], refs[4], refs[5]
        for n in range(lo_ref.shape[-1] // tile):
            cols = pl.ds(n * tile, tile)
            store_halves(lo_ref, hi_ref, cols, dot_nn(act_mix, down_ref[0, :, cols]))


def backward_body(tile, based, rows_ref, a_ref, u_ref, down_ref, *refs):
    base, refs = refs[:based], refs[based:]
    more = len(refs) > 2
    dg_ref, du_ref = refs[2:4] if more else refs
    d_mix = dot_nt(rows_ref[0], down_ref[0])
    if based:
        d_mix = base[0][0] + d_mix
    d_gate, d_up = act_backward(d_mix, a_ref[0], u_ref[0])
    dg_ref[0] = d_gate
    du_ref[0] = d_up
    if more:
        gate_ref, up_ref = refs[:2]
        lo_ref, hi_ref = refs[4:]
        for n in range(lo_ref.shape[-1] // tile):
            cols = pl.ds(n * tile, tile)
            store_halves(lo_ref, hi_ref, cols, dot_nn(d_gate, gate_ref[0, :, cols]) + dot_nn(d_up, up_ref[0, :, cols]))


def expert_specs(rows, ff):
    n_exp, n_rows, dim = rows.shape
    w_spec, r_spec, f_spec, h_spec = leading(ff, dim), leading(n_rows, dim), leading(n_rows, ff), leading(n_rows // 2, dim)
    f_shape = jax.ShapeDtypeStruct((n_exp, n_rows, ff), BF16)
    h_shape = jax.ShapeDtypeStruct((n_exp, n_rows // 2, dim), BF16)
    return w_spec, r_spec, f_spec, f_shape, h_spec, h_shape


def expert_cost(rows, ff, dots):
    n_exp, n_rows, dim = rows.shape
    return cost(2 * dots * n_exp * n_rows * dim * ff, 2 * n_exp * (dots * ff * dim + 2 * n_rows * dim))


def expert_forward(rows, gate_t, up_t, down=None):
    ff = gate_t.shape[1]
    w_spec, r_spec, f_spec, f_shape, h_spec, h_shape = expert_specs(rows, ff)
    more = down is not None
    return pl.pallas_call(
        functools.partial(forward_body, 1024),
        grid=(rows.shape[0],),
        in_specs=[r_spec, w_spec, w_spec] + [w_spec] * more,
        out_specs=[f_spec] * 3 + [h_spec] * (2 * more),
        out_shape=[f_shape] * 3 + [h_shape] * (2 * more),
        compiler_params=params(1),
        cost_estimate=expert_cost(rows, ff, 2 + more),
        name="expert_forward",
    )(rows, gate_t, up_t, *((down,) if more else ()))


def expert_backward(rows, a, u, down, weights=(), start=0, base=None):
    n_exp, n_rows, width = rows.shape
    ff, dim = down.shape[1:]
    more, sums = len(weights), () if base is None else (base,)
    w_spec, f_spec, h_spec = leading(ff, dim), leading(n_rows, ff), leading(n_rows // 2, dim)
    down_spec = pl.BlockSpec((1, ff, width), lambda e: (e, 0, start // width))
    f_shape, h_shape = (jax.ShapeDtypeStruct(shape, BF16) for shape in ((n_exp, n_rows, ff), (n_exp, n_rows // 2, dim)))
    return pl.pallas_call(
        functools.partial(backward_body, 1024, len(sums)),
        grid=(n_exp,),
        in_specs=[leading(n_rows, width), f_spec, f_spec, down_spec] + [f_spec] * len(sums) + [w_spec] * more,
        out_specs=[f_spec] * 2 + [h_spec] * more,
        out_shape=[f_shape] * 2 + [h_shape] * more,
        compiler_params=params(1),
        cost_estimate=expert_cost(rows, ff, 1 + more),
        name="expert_backward",
    )(rows, a, u, down, *sums, *weights)


def chunk_body(rows_ref, down_ref, *refs):
    d_mix = dot_nt(rows_ref[0], down_ref[0])
    refs[-1][0] = d_mix if len(refs) == 1 else refs[0][0] + d_mix


def backward_chunk(rows, start, down, base):
    n_exp, n_rows, width = rows.shape
    ff = down.shape[1]
    sums = () if base is None else (base,)
    f_spec = leading(n_rows, ff)
    return pl.pallas_call(
        chunk_body,
        grid=(n_exp,),
        in_specs=[leading(n_rows, width), pl.BlockSpec((1, ff, width), lambda e: (e, 0, start // width))] + [f_spec] * len(sums),
        out_specs=f_spec,
        out_shape=jax.ShapeDtypeStruct((n_exp, n_rows, ff), F32),
        compiler_params=params(1),
        cost_estimate=expert_cost(rows, ff, 1),
        name="backward_chunk",
    )(rows, down, *sums)


def wgrad_body(n_parts, adds, *refs):
    small, wide, base = refs[:n_parts], refs[n_parts:2 * n_parts], refs[2 * n_parts:-3]
    out_ref, small_all, wide_all = refs[-3:]
    if n_parts == 1:
        sums = dot_tn(small[0][0], wide[0][0])
    else:
        start = 0
        for part in range(n_parts):
            span = pl.ds(start, small[part].shape[1])
            start += small[part].shape[1]

            @pl.when(pl.program_id(1) == 0)
            def _():
                small_all[span, :] = small[part][0]

            wide_all[span, :] = wide[part][0]
        sums = dot_tn(small_all[...], wide_all[...])
    out_ref[0] = base[0][0] + sums if adds else sums


def weight_grad(small, wide, base=None, adds=False, start=0, width=None, tile=2048):
    n_exp, _, ff = small[0].shape
    dim = wide[0].shape[2]
    width = width or dim
    tile = min(tile, width)
    total = sum(s.shape[1] for s in small)
    skip = start // tile

    def wide_spec(w):
        first = skip if w.shape[2] == dim else 0
        return pl.BlockSpec((1, w.shape[1], tile), lambda e, n: (e, 0, n + first))

    out_spec = pl.BlockSpec((1, ff, tile), lambda e, n: (e, 0, n + skip))
    base_specs = [] if base is None else [out_spec if adds else pl.BlockSpec(memory_space=pl.ANY)]
    stacked = total if len(small) > 1 else 16
    return pl.pallas_call(
        functools.partial(wgrad_body, len(small), adds),
        grid=(n_exp, width // tile),
        in_specs=[leading(s.shape[1], ff) for s in small] + [wide_spec(w) for w in wide] + base_specs,
        out_specs=out_spec,
        out_shape=jax.ShapeDtypeStruct((n_exp, ff, dim), F32),
        input_output_aliases={} if base is None else {2 * len(small): 0},
        scratch_shapes=[pltpu.VMEM((stacked, ff), BF16), pltpu.VMEM((stacked, tile), BF16)],
        compiler_params=params(2),
        cost_estimate=cost(2 * n_exp * total * width * ff, n_exp * (4 * ff * width + 2 * total * (width + ff))),
        name="weight_grad",
    )(*small, *wide, *(() if base is None else (base,)))


def fill_hot(tgt_ref, first_slot, *hots):
    chunk = 128
    slots = hots[0].shape[1]

    @pl.loop(0, hots[0].shape[0] // chunk)
    def _(c):
        rows = pl.ds(pl.multiple_of(c * chunk, chunk), chunk)
        lanes = lax.broadcasted_iota(jnp.int32, (chunk, slots), 1) + first_slot
        first, second = (col(tgt_ref[rows, :], k) == lanes for k in range(2))
        if len(hots) == 2:
            hots[0][rows, :] = first.astype(F32).astype(BF16)
            hots[1][rows, :] = second.astype(F32).astype(BF16)
        else:
            hots[0][rows, :] = (first | second).astype(F32).astype(BF16)


def stack_rows(rets, rows):
    n_exp, cap, tile = rets[0].shape
    for q, ret in enumerate(rets):
        rows[pl.ds(q * n_exp * cap, n_exp * cap), :] = ret[...].reshape(n_exp * cap, tile)
    return rows[...]


def combine_body(n_ret, first_slot, last, tgt_ref, p_ref, dout_ref, in_ref, *refs):
    rets, refs = refs[:n_ret], refs[n_ret:]
    if last:
        ids_ref, dgate_in, out_ref, dlog_ref, hot_a, hot_b, rows, dgate_ref = refs
    else:
        out_ref, dgate_ref, hot_a, hot_b, rows = refs

    @pl.when(pl.program_id(0) == 0)
    def _():
        fill_hot(tgt_ref, first_slot, hot_a, hot_b)
        dgate_ref[...] = dgate_in[...] if last else jnp.zeros_like(dgate_ref)

    stacked = stack_rows(rets, rows)
    first, second = dot_nn(hot_a[...], stacked), dot_nn(hot_b[...], stacked)
    dout = dout_ref[...].astype(F32)
    out_ref[...] = (in_ref[...].astype(F32) + (col(p_ref, 0) * first + col(p_ref, 1) * second)).astype(out_ref.dtype)
    for k, rows_k in enumerate((first, second)):
        dgate_ref[:, k * LANES:(k + 1) * LANES] += fold_lanes(rows_k * dout)

    if last:
        @pl.when(pl.program_id(0) == pl.num_programs(0) - 1)
        def _():
            p_a, p_b = col(p_ref, 0), col(p_ref, 1)
            g_a, g_b = lane_total(dgate_ref, 0), lane_total(dgate_ref, 1)
            mean = p_a * g_a + p_b * g_b
            expert = lax.broadcasted_iota(jnp.int32, dlog_ref.shape, 1)
            d_a = jnp.where(col(ids_ref, 0) == expert, p_a * (g_a - mean), 0.0)
            d_b = jnp.where(col(ids_ref, 1) == expert, p_b * (g_b - mean), 0.0)
            dlog_ref[...] = (d_a + d_b).astype(BF16)


def combine(tgt, gate_probs, dout, base, rets, first_slot, ids=None, dgates=None, experts=0, tile=512):
    tokens, dim = base.shape
    n_exp, cap, _ = rets[0].shape
    slots = len(rets) * n_exp * cap
    last = ids is not None
    full, cols, ret_spec = whole(tokens, 2), striped(tokens, tile), striped(n_exp, cap, tile)
    wide = whole(tokens, 2 * LANES)
    side = whole(tokens, experts) if last else wide
    side_shape = jax.ShapeDtypeStruct((tokens, experts), BF16) if last else jax.ShapeDtypeStruct((tokens, 2 * LANES), F32)
    return pl.pallas_call(
        functools.partial(combine_body, len(rets), first_slot, last),
        grid=(dim // tile,),
        in_specs=[full, full, cols, cols] + [ret_spec] * len(rets) + [full, wide] * last,
        out_specs=[cols, side],
        out_shape=[jax.ShapeDtypeStruct((tokens, dim), BF16 if last else F32), side_shape],
        scratch_shapes=[pltpu.VMEM((tokens, slots), BF16), pltpu.VMEM((tokens, slots), BF16), pltpu.VMEM((slots, tile), BF16)] + [pltpu.VMEM((tokens, 2 * LANES), F32)] * last,
        compiler_params=params(1),
        cost_estimate=cost(4 * tokens * slots * dim, 2 * (4 * tokens + slots) * dim),
        name="combine",
    )(tgt, gate_probs, dout, base, *rets, *((ids, dgates) if last else ()))


def near_body(n_ret, tgt_ref, *refs):
    rets, (out_ref, hot, rows) = refs[:n_ret], refs[n_ret:]

    @pl.when(pl.program_id(0) == 0)
    def _():
        fill_hot(tgt_ref, 0, hot)

    out_ref[...] = dot_nn(hot[...], stack_rows(rets, rows))


def near_rows(tgt, rets, tile=512):
    tokens = tgt.shape[0]
    n_exp, cap, dim = rets[0].shape
    slots = len(rets) * n_exp * cap
    return pl.pallas_call(
        functools.partial(near_body, len(rets)),
        grid=(dim // tile,),
        in_specs=[whole(tokens, 2)] + [striped(n_exp, cap, tile)] * len(rets),
        out_specs=striped(tokens, tile),
        out_shape=jax.ShapeDtypeStruct((tokens, dim), F32),
        scratch_shapes=[pltpu.VMEM((tokens, slots), BF16), pltpu.VMEM((slots, tile), BF16)],
        compiler_params=params(1),
        cost_estimate=cost(2 * tokens * slots * dim, 2 * (2 * tokens + slots) * dim),
        name="near_rows",
    )(tgt, *rets)


def finish_body(n_ret, first_slot, tgt_ref, dlog_ref, stat_ref, router_ref, gain_ref, x_ref, dout_ref, near_ref, *refs):
    rets = refs[:n_ret]
    gx_ref, ggain_ref, gbias_ref, hot, rows, d_hid, row_sums, means = refs[n_ret:]
    phase, n = pl.program_id(0), pl.program_id(1)
    tile = rets[0].shape[2]
    dim = d_hid.shape[1]
    cols = pl.ds(pl.multiple_of(n * tile, tile), tile)

    @pl.when((phase == 0) & (n == 0))
    def _():
        fill_hot(tgt_ref, first_slot, hot)
        row_sums[...] = jnp.zeros_like(row_sums)

    inv_std = col(stat_ref, 1)
    normed = (x_ref[...].astype(F32) - col(stat_ref, 0)) * inv_std

    @pl.when(phase == 0)
    def _():
        far = dot_nn(hot[...], stack_rows(rets, rows))
        rounded = (near_ref[...] + far + dot_nn(dlog_ref[...], router_ref[...])).astype(BF16)
        d_hid[:, cols] = rounded
        d_h = rounded.astype(F32)
        weighted = d_h * normed
        ggain_ref[...] = jnp.sum(weighted, axis=0, keepdims=True)
        gbias_ref[...] = jnp.sum(d_h, axis=0, keepdims=True)
        for k, rows_k in enumerate((d_h, weighted)):
            row_sums[:, k * LANES:(k + 1) * LANES] += fold_lanes(rows_k * gain_ref[...])

    @pl.when((phase == 1) & (n == 0))
    def _():
        for k in range(2):
            means[:, k:k + 1] = lane_total(row_sums, k) * (1.0 / dim)

    @pl.when(phase == 1)
    def _():
        d_norm = d_hid[:, cols].astype(F32) * gain_ref[...]
        mean_dn, mean_dnn = col(means, 0), col(means, 1)
        gx_ref[...] = (dout_ref[...].astype(F32) + inv_std * (d_norm - mean_dn - normed * mean_dnn)).astype(BF16)


def finish(tgt, d_logits, stats, router_t, gain, x_loc, dout, near, rets, first_slot, tile=512):
    tokens, dim = x_loc.shape
    experts = d_logits.shape[1]
    n_exp, cap, _ = rets[0].shape
    slots = len(rets) * n_exp * cap
    last = dim // tile - 1

    def early(p, n):
        return jnp.where(p == 0, n, last)

    full = whole(tokens, 2)
    both = pl.BlockSpec((tokens, tile), lambda p, n: (0, n))
    late = pl.BlockSpec((tokens, tile), lambda p, n: (0, n * p))
    line = pl.BlockSpec((1, tile), lambda p, n: (0, n))
    early_line = pl.BlockSpec((1, tile), lambda p, n: (0, early(p, n)))
    ret_spec = pl.BlockSpec((n_exp, cap, tile), lambda p, n: (0, 0, early(p, n)))
    return pl.pallas_call(
        functools.partial(finish_body, len(rets), first_slot),
        grid=(2, dim // tile),
        in_specs=[full, whole(tokens, experts), full, pl.BlockSpec((experts, tile), lambda p, n: (0, n)), line, both, late]
        + [pl.BlockSpec((tokens, tile), lambda p, n: (0, early(p, n)))] + [ret_spec] * len(rets),
        out_specs=[late, early_line, early_line],
        out_shape=[jax.ShapeDtypeStruct((tokens, dim), BF16), jax.ShapeDtypeStruct((1, dim), F32), jax.ShapeDtypeStruct((1, dim), F32)],
        scratch_shapes=[pltpu.VMEM((tokens, slots), BF16), pltpu.VMEM((slots, tile), BF16), pltpu.VMEM((tokens, dim), BF16), pltpu.VMEM((tokens, 2 * LANES), F32), pltpu.VMEM((tokens, 2), F32)],
        compiler_params=params(2),
        cost_estimate=cost(2 * tokens * slots * dim, 2 * (7 * tokens + slots) * dim),
        name="finish",
    )(tgt, d_logits, stats, router_t, gain, x_loc, dout, near, *rets)


def solution(mesh):
    n_dp, n_ep = mesh.shape["dp"], mesh.shape["ep"]
    tok_spec = P(("dp", "ep"), None)
    exp_spec = P("ep", None, None)

    def swap(value, bits):
        return lax.ppermute(value, "ep", [(j, j ^ bits) for j in range(n_ep)])

    def cross(value):
        return lax.ppermute(value, "dp", [(i, i ^ 1) for i in range(n_dp)])

    def total(value):
        value = value + swap(value, 1)
        value = value + cross(value)
        return value + swap(value, 2)

    def local_step(x_loc, ln_gain, ln_bias, w_router, w_gate, w_up, w_down, ids_loc, slots_loc, dout):
        tokens, dim = x_loc.shape
        experts = w_router.shape[1]
        n_exp = w_gate.shape[0]
        cap = capacity_for(tokens, experts, ids_loc.shape[1])
        local = n_exp * cap
        j = lax.axis_index("ep")
        gate_t, up_t = jnp.swapaxes(w_gate, 1, 2), jnp.swapaxes(w_up, 1, 2)
        base = (j * local).astype(jnp.int32)[None]

        def gather(routes, sources, scaled=False):
            rows, *hot = gather_call(True, scaled, sources, n_exp, cap, (base,) + routes)
            return rows, hot

        def gather_more(hot, sources, scaled=True):
            return gather_call(False, scaled, sources, n_exp, cap, hot)

        hidden, stats, logits = norm_router(x_loc, ln_gain[None], ln_bias[None], w_router.T)
        h_x, h_c, g_0 = swap(hidden, 2), swap(hidden, 1), cross(hidden)

        ids_t, slots_t, logits_t = ids_loc.T, slots_loc.T, logits.T
        kept = slots_t >= 0
        target = jnp.where(kept, ids_t * cap + slots_t, -1)
        picked = jnp.sum(jnp.where(ids_t[:, None, :] == jnp.arange(experts)[None, :, None], logits_t[None], 0.0), axis=1)
        probs = jax.nn.softmax(picked, axis=0)
        route = jnp.concatenate([target.astype(F32), probs, jnp.zeros((4, tokens), F32)])
        r_x, r_c, r_0 = swap(route, 2), swap(route, 1), cross(route)
        chunks = [(dim // 4 * s, dim // 4 * w) for s, w in ((0, 2), (2, 1), (3, 1))]
        d_cols = [lax.slice_in_dim(dout, s, s + w, axis=1) for s, w in chunks]
        d_x = [swap(part, 2) for part in d_cols]
        d_c, e_0 = swap(dout, 1), cross(dout)

        rows_a, hot_a = gather((route, r_c), (hidden, h_c))
        act_a = expert_forward(rows_a, gate_t, up_t, w_down)
        grads_a = gather_more(hot_a, (dout, d_c))
        back_a = expert_backward(grads_a, act_a[0], act_a[1], w_down, (gate_t, up_t))
        y_c = swap(act_a[4], 1)
        d_rows_c = swap(back_a[3], 1)
        tgt = jnp.where(kept, (ids_t // n_exp ^ j) * local + (ids_t % n_exp) * cap + slots_t, -1).T
        p_cols = probs.T
        moe_near, dgate_near = combine(tgt, p_cols, dout, x_loc, (act_a[3], y_c), 0)
        d_near = near_rows(tgt, (back_a[2], d_rows_c))

        h_xc, r_xc = swap(h_x, 1), swap(r_x, 1)
        g_2, r_2 = cross(h_x), cross(r_x)
        rows_b, hot_b = gather((r_x, r_xc), (h_x, h_xc))
        act_b = expert_forward(rows_b, gate_t, up_t, w_down)
        y_home = (swap(act_b[3], 2), swap(act_b[4], 3))

        grads_b, d_mix, e_2 = [], None, []
        for c, (start, width) in enumerate(chunks):
            grads_b.append(gather_more(hot_b, (d_x[c], swap(d_x[c], 1))))
            e_2.append(cross(d_x[c]))
            if c < len(chunks) - 1:
                d_mix = backward_chunk(grads_b[c], start, w_down, d_mix)
            else:
                back_b = expert_backward(grads_b[c], act_b[0], act_b[1], w_down, (gate_t, up_t), start, d_mix)
        d_home = (swap(back_b[2], 2), swap(back_b[3], 3))

        g_1, r_1, e_1 = swap(g_0, 1), swap(r_0, 1), swap(e_0, 1)
        grads_o, hot_o = gather((r_0, r_1), (e_0, e_1), True)
        rows_o = gather_more(hot_o, (g_0, g_1), False)
        act_o = expert_forward(rows_o, gate_t, up_t)

        back_o = expert_backward(grads_o, act_o[0], act_o[1], w_down)
        grad_gate = weight_grad((back_a[0], back_b[0], back_o[0]), (rows_a, rows_b, rows_o))
        grad_up = weight_grad((back_a[1], back_b[1], back_o[1]), (rows_a, rows_b, rows_o))

        g_3, r_3 = swap(g_2, 1), swap(r_2, 1)
        rows_q, hot_q = gather((r_2, r_3), (g_2, g_3))
        act_q = expert_forward(rows_q, gate_t, up_t)

        moe_out, d_logits = combine(tgt, p_cols, dout, moe_near, y_home, 2 * local, ids_loc, dgate_near, experts)
        grad_router = total(jnp.einsum("te,tm->em", d_logits, hidden, preferred_element_type=F32))

        grad_down, d_mix = None, None
        for c, (start, width) in enumerate(chunks):
            e_3 = swap(e_2[c], 1)
            grads_q = gather_more(hot_q, (e_2[c], e_3))
            if c < len(chunks) - 1:
                d_mix = backward_chunk(grads_q, start, w_down, d_mix)
            else:
                back_q = expert_backward(grads_q, act_q[0], act_q[1], w_down, (), start, d_mix)
            grad_down = weight_grad((act_a[2], act_b[2], act_o[2], act_q[2]), (grads_a, grads_b[c], grads_o, grads_q), grad_down, False, start, width)
        grad_gate = weight_grad((back_q[0],), (rows_q,), grad_gate, True)
        grad_up = weight_grad((back_q[1],), (rows_q,), grad_up, True)

        grad_x, g_gain, g_bias = finish(tgt, d_logits, stats, w_router.T, ln_gain[None], x_loc, dout, d_near, d_home, 2 * local)
        g_norm = total(jnp.concatenate([g_gain, g_bias]))
        return (moe_out, grad_x, g_norm[0], g_norm[1], grad_router.T, jnp.swapaxes(grad_gate, 1, 2), jnp.swapaxes(grad_up, 1, 2), grad_down)

    return jax.shard_map(local_step, mesh=mesh, in_specs=(tok_spec, P(None), P(None), P(None, None), exp_spec, exp_spec, exp_spec, tok_spec, tok_spec, tok_spec), out_specs=(tok_spec, tok_spec, P(None), P(None), P(None, None), exp_spec, exp_spec, exp_spec), check_vma=False)
```

```python
import functools

import jax
import jax.numpy as jnp
from jax import lax
from jax.experimental import pallas as pl
from jax.experimental.pallas import tpu as pltpu
from jax.sharding import PartitionSpec as P


LN_EPS = 1e-5
F32 = jnp.float32
BF16 = jnp.bfloat16
LANES = 128
VMEM_LIMIT = 62 * 1024 * 1024


def capacity_for(tokens_dev, experts, n_top):
    return 8 * ((5 * tokens_dev * n_top + 32 * experts - 1) // (32 * experts))


def params(n_axes):
    return pltpu.CompilerParams(dimension_semantics=("arbitrary",) * n_axes, vmem_limit_bytes=VMEM_LIMIT)


def cost(flops, nbytes):
    return pl.CostEstimate(flops=int(flops), bytes_accessed=int(nbytes), transcendentals=0)


def dot(lhs, rhs, l_dim, r_dim):
    return lax.dot_general(lhs, rhs, (((l_dim,), (r_dim,)), ((), ())), preferred_element_type=F32)


def dot_nn(lhs, rhs):
    return dot(lhs, rhs, 1, 0)


def dot_nt(lhs, rhs):
    return dot(lhs, rhs, 1, 1)


def dot_tn(lhs, rhs):
    return dot(lhs, rhs, 0, 0)


def col(ref, k):
    return ref[:, k:k + 1]


def fold_lanes(value):
    parts = [value[:, k:k + LANES] for k in range(0, value.shape[1], LANES)]
    return functools.reduce(jnp.add, parts)


def lane_total(ref, k):
    return jnp.sum(ref[:, k * LANES:(k + 1) * LANES], axis=1, keepdims=True)


def whole(*shape):
    return pl.BlockSpec(shape, lambda *_: (0,) * len(shape))


def leading(*shape):
    return pl.BlockSpec((1,) + shape, lambda e, *_: (e, 0, 0))


def striped(*shape):
    return pl.BlockSpec(shape, lambda n: (0,) * (len(shape) - 1) + (n,))


def norm_body(x_ref, gain_ref, bias_ref, router_ref, hid_ref, stat_ref, logit_ref):
    x_f = x_ref[...].astype(F32)
    mean = jnp.mean(x_f, axis=-1, keepdims=True)
    centered = x_f - mean
    inv_std = lax.rsqrt(jnp.mean(centered * centered, axis=-1, keepdims=True) + LN_EPS)
    hidden = (centered * inv_std * gain_ref[...] + bias_ref[...]).astype(BF16)
    hid_ref[...] = hidden
    stat_ref[...] = jnp.concatenate([mean, inv_std], axis=1)
    logit_ref[...] = dot_nt(hidden, router_ref[...])


def norm_router(x_loc, gain, bias, router_t, tile=256):
    tokens, dim = x_loc.shape
    experts = router_t.shape[0]
    line = whole(1, dim)

    def by_row(width):
        return pl.BlockSpec((tile, width), lambda t: (t, 0))

    return pl.pallas_call(
        norm_body,
        grid=(tokens // tile,),
        in_specs=[by_row(dim), line, line, whole(experts, dim)],
        out_specs=[by_row(dim), by_row(2), by_row(experts)],
        out_shape=[jax.ShapeDtypeStruct((tokens, dim), BF16), jax.ShapeDtypeStruct((tokens, 2), F32), jax.ShapeDtypeStruct((tokens, experts), F32)],
        compiler_params=params(1),
        cost_estimate=cost(20 * tokens * dim, 4 * tokens * dim),
        name="norm_router",
    )(x_loc, gain, bias, router_t)


def gather_body(n_src, first_use, scaled, *refs):
    if first_use:
        base_ref, routes, srcs, (out_ref, hot_ref, p_ref) = refs[0], refs[1:n_src + 1], refs[n_src + 1:-3], refs[-3:]
    else:
        hot_ref, p_ref, srcs, out_ref = refs[0], refs[1], refs[2:-1], refs[-1]
    r, n = pl.program_id(0), pl.program_id(1)
    n_exp, cap, _ = out_ref.shape
    tokens = hot_ref.shape[2]

    for q in range(n_src):
        if first_use:
            @pl.when((r == q) & (n == 0))
            def _():
                id_a, id_b, p_a, p_b = (routes[q][k:k + 1, :] for k in range(4))
                for e in range(n_exp):
                    span = pl.ds(e * cap, cap)
                    slot = (lax.broadcasted_iota(jnp.int32, (cap, tokens), 0) + (base_ref[0] + e * cap)).astype(F32)
                    first, second = id_a == slot, id_b == slot
                    hot_ref[0, span, :] = (first | second).astype(F32).astype(BF16)
                    p_ref[0, span, :] = jnp.sum(jnp.where(first, p_a, jnp.where(second, p_b, 0.0)), axis=1, keepdims=True)

        @pl.when(r == q)
        def _():
            rows = dot_nn(hot_ref[0], srcs[q][...])
            if scaled:
                rows = rows * p_ref[0]
            out_ref[...] = rows.astype(BF16).reshape(out_ref.shape)


def gather_call(first_use, scaled, sources, n_exp, cap, args, tile=2048):
    n_src = len(sources)
    tokens, dim = sources[0].shape
    tile = min(tile, dim)
    slots = n_exp * cap
    last = dim // tile - 1

    def src_map(q, r, n):
        return (0, jnp.where(r == q, n, jnp.where(r < q, 0, last)))

    hot_specs = [leading(slots, tokens), leading(slots, 1)]
    hot_shapes = [jax.ShapeDtypeStruct((n_src, slots, tokens), BF16), jax.ShapeDtypeStruct((n_src, slots, 1), F32)]
    arg_specs = [pl.BlockSpec(memory_space=pltpu.SMEM)] + [whole(*t.shape) for t in args[1:]] if first_use else hot_specs
    out_spec = pl.BlockSpec((n_exp, cap, tile), lambda r, n: (0, r, n))
    out_shape = jax.ShapeDtypeStruct((n_exp, n_src * cap, dim), BF16)
    return pl.pallas_call(
        functools.partial(gather_body, n_src, first_use, scaled),
        grid=(n_src, dim // tile),
        in_specs=arg_specs + [pl.BlockSpec((tokens, tile), functools.partial(src_map, q)) for q in range(n_src)],
        out_specs=[out_spec] + hot_specs if first_use else out_spec,
        out_shape=[out_shape] + hot_shapes if first_use else out_shape,
        compiler_params=params(2),
        cost_estimate=cost(2 * n_src * slots * tokens * dim, 2 * n_src * (tokens + slots) * dim),
        name="gather_rows",
    )(*args, *sources)


def act_forward(rows, gate, up):
    pre_gate = dot_nt(rows, gate).astype(BF16)
    pre_up = dot_nt(rows, up).astype(BF16)
    gate_f = pre_gate.astype(F32)
    act_mix = (gate_f * jax.nn.sigmoid(gate_f) * pre_up.astype(F32)).astype(BF16)
    return pre_gate, pre_up, act_mix


def act_backward(d_mix, pre_gate, pre_up):
    d_mix = d_mix.astype(BF16).astype(F32)
    gate_f = pre_gate.astype(F32)
    sig = jax.nn.sigmoid(gate_f)
    d_gate = (d_mix * pre_up.astype(F32) * sig * (1.0 + gate_f * (1.0 - sig))).astype(BF16)
    d_up = (d_mix * gate_f * sig).astype(BF16)
    return d_gate, d_up


def store_halves(lo_ref, hi_ref, cols, value):
    half = lo_ref.shape[1]
    lo_ref[0, :, cols] = value[:half].astype(BF16)
    hi_ref[0, :, cols] = value[half:].astype(BF16)


def forward_body(tile, rows_ref, gate_ref, up_ref, *refs):
    a_ref, u_ref, m_ref = refs[-5:-2] if len(refs) == 6 else refs
    pre_gate, pre_up, act_mix = act_forward(rows_ref[0], gate_ref[0], up_ref[0])
    a_ref[0] = pre_gate
    u_ref[0] = pre_up
    m_ref[0] = act_mix
    if len(refs) == 6:
        down_ref, lo_ref, hi_ref = refs[0], refs[4], refs[5]
        for n in range(lo_ref.shape[-1] // tile):
            cols = pl.ds(n * tile, tile)
            store_halves(lo_ref, hi_ref, cols, dot_nn(act_mix, down_ref[0, :, cols]))


def backward_body(tile, based, rows_ref, a_ref, u_ref, down_ref, *refs):
    base, refs = refs[:based], refs[based:]
    more = len(refs) > 2
    dg_ref, du_ref = refs[2:4] if more else refs
    d_mix = dot_nt(rows_ref[0], down_ref[0])
    if based:
        d_mix = base[0][0] + d_mix
    d_gate, d_up = act_backward(d_mix, a_ref[0], u_ref[0])
    dg_ref[0] = d_gate
    du_ref[0] = d_up
    if more:
        gate_ref, up_ref = refs[:2]
        lo_ref, hi_ref = refs[4:]
        for n in range(lo_ref.shape[-1] // tile):
            cols = pl.ds(n * tile, tile)
            store_halves(lo_ref, hi_ref, cols, dot_nn(d_gate, gate_ref[0, :, cols]) + dot_nn(d_up, up_ref[0, :, cols]))


def expert_specs(rows, ff):
    n_exp, n_rows, dim = rows.shape
    w_spec, r_spec, f_spec, h_spec = leading(ff, dim), leading(n_rows, dim), leading(n_rows, ff), leading(n_rows // 2, dim)
    f_shape = jax.ShapeDtypeStruct((n_exp, n_rows, ff), BF16)
    h_shape = jax.ShapeDtypeStruct((n_exp, n_rows // 2, dim), BF16)
    return w_spec, r_spec, f_spec, f_shape, h_spec, h_shape


def expert_cost(rows, ff, dots):
    n_exp, n_rows, dim = rows.shape
    return cost(2 * dots * n_exp * n_rows * dim * ff, 2 * n_exp * (dots * ff * dim + 2 * n_rows * dim))


def expert_forward(rows, gate_t, up_t, down=None):
    ff = gate_t.shape[1]
    w_spec, r_spec, f_spec, f_shape, h_spec, h_shape = expert_specs(rows, ff)
    more = down is not None
    return pl.pallas_call(
        functools.partial(forward_body, 1024),
        grid=(rows.shape[0],),
        in_specs=[r_spec, w_spec, w_spec] + [w_spec] * more,
        out_specs=[f_spec] * 3 + [h_spec] * (2 * more),
        out_shape=[f_shape] * 3 + [h_shape] * (2 * more),
        compiler_params=params(1),
        cost_estimate=expert_cost(rows, ff, 2 + more),
        name="expert_forward",
    )(rows, gate_t, up_t, *((down,) if more else ()))


def expert_backward(rows, a, u, down, weights=(), start=0, base=None):
    n_exp, n_rows, width = rows.shape
    ff, dim = down.shape[1:]
    more, sums = len(weights), () if base is None else (base,)
    w_spec, f_spec, h_spec = leading(ff, dim), leading(n_rows, ff), leading(n_rows // 2, dim)
    down_spec = pl.BlockSpec((1, ff, width), lambda e: (e, 0, start // width))
    f_shape, h_shape = (jax.ShapeDtypeStruct(shape, BF16) for shape in ((n_exp, n_rows, ff), (n_exp, n_rows // 2, dim)))
    return pl.pallas_call(
        functools.partial(backward_body, 1024, len(sums)),
        grid=(n_exp,),
        in_specs=[leading(n_rows, width), f_spec, f_spec, down_spec] + [f_spec] * len(sums) + [w_spec] * more,
        out_specs=[f_spec] * 2 + [h_spec] * more,
        out_shape=[f_shape] * 2 + [h_shape] * more,
        compiler_params=params(1),
        cost_estimate=expert_cost(rows, ff, 1 + more),
        name="expert_backward",
    )(rows, a, u, down, *sums, *weights)


def chunk_body(rows_ref, down_ref, *refs):
    d_mix = dot_nt(rows_ref[0], down_ref[0])
    refs[-1][0] = d_mix if len(refs) == 1 else refs[0][0] + d_mix


def backward_chunk(rows, start, down, base):
    n_exp, n_rows, width = rows.shape
    ff = down.shape[1]
    sums = () if base is None else (base,)
    f_spec = leading(n_rows, ff)
    return pl.pallas_call(
        chunk_body,
        grid=(n_exp,),
        in_specs=[leading(n_rows, width), pl.BlockSpec((1, ff, width), lambda e: (e, 0, start // width))] + [f_spec] * len(sums),
        out_specs=f_spec,
        out_shape=jax.ShapeDtypeStruct((n_exp, n_rows, ff), F32),
        compiler_params=params(1),
        cost_estimate=expert_cost(rows, ff, 1),
        name="backward_chunk",
    )(rows, down, *sums)


def wgrad_body(n_parts, adds, *refs):
    small, wide, base = refs[:n_parts], refs[n_parts:2 * n_parts], refs[2 * n_parts:-3]
    out_ref, small_all, wide_all = refs[-3:]
    if n_parts == 1:
        sums = dot_tn(small[0][0], wide[0][0])
    else:
        start = 0
        for part in range(n_parts):
            span = pl.ds(start, small[part].shape[1])
            start += small[part].shape[1]

            @pl.when(pl.program_id(1) == 0)
            def _():
                small_all[span, :] = small[part][0]

            wide_all[span, :] = wide[part][0]
        sums = dot_tn(small_all[...], wide_all[...])
    out_ref[0] = base[0][0] + sums if adds else sums


def weight_grad(small, wide, base=None, adds=False, start=0, width=None, tile=2048):
    n_exp, _, ff = small[0].shape
    dim = wide[0].shape[2]
    width = width or dim
    tile = min(tile, width)
    total = sum(s.shape[1] for s in small)
    skip = start // tile

    def wide_spec(w):
        first = skip if w.shape[2] == dim else 0
        return pl.BlockSpec((1, w.shape[1], tile), lambda e, n: (e, 0, n + first))

    out_spec = pl.BlockSpec((1, ff, tile), lambda e, n: (e, 0, n + skip))
    base_specs = [] if base is None else [out_spec if adds else pl.BlockSpec(memory_space=pl.ANY)]
    stacked = total if len(small) > 1 else 16
    return pl.pallas_call(
        functools.partial(wgrad_body, len(small), adds),
        grid=(n_exp, width // tile),
        in_specs=[leading(s.shape[1], ff) for s in small] + [wide_spec(w) for w in wide] + base_specs,
        out_specs=out_spec,
        out_shape=jax.ShapeDtypeStruct((n_exp, ff, dim), F32),
        input_output_aliases={} if base is None else {2 * len(small): 0},
        scratch_shapes=[pltpu.VMEM((stacked, ff), BF16), pltpu.VMEM((stacked, tile), BF16)],
        compiler_params=params(2),
        cost_estimate=cost(2 * n_exp * total * width * ff, n_exp * (4 * ff * width + 2 * total * (width + ff))),
        name="weight_grad",
    )(*small, *wide, *(() if base is None else (base,)))


def fill_hot(tgt_ref, first_slot, *hots):
    chunk = 128
    slots = hots[0].shape[1]

    @pl.loop(0, hots[0].shape[0] // chunk)
    def _(c):
        rows = pl.ds(pl.multiple_of(c * chunk, chunk), chunk)
        lanes = lax.broadcasted_iota(jnp.int32, (chunk, slots), 1) + first_slot
        first, second = (col(tgt_ref[rows, :], k) == lanes for k in range(2))
        if len(hots) == 2:
            hots[0][rows, :] = first.astype(F32).astype(BF16)
            hots[1][rows, :] = second.astype(F32).astype(BF16)
        else:
            hots[0][rows, :] = (first | second).astype(F32).astype(BF16)


def stack_rows(rets, rows):
    n_exp, cap, tile = rets[0].shape
    for q, ret in enumerate(rets):
        rows[pl.ds(q * n_exp * cap, n_exp * cap), :] = ret[...].reshape(n_exp * cap, tile)
    return rows[...]


def combine_body(n_ret, first_slot, last, tgt_ref, p_ref, dout_ref, in_ref, *refs):
    rets, refs = refs[:n_ret], refs[n_ret:]
    if last:
        ids_ref, dgate_in, out_ref, dlog_ref, hot_a, hot_b, rows, dgate_ref = refs
    else:
        out_ref, dgate_ref, hot_a, hot_b, rows = refs

    @pl.when(pl.program_id(0) == 0)
    def _():
        fill_hot(tgt_ref, first_slot, hot_a, hot_b)
        dgate_ref[...] = dgate_in[...] if last else jnp.zeros_like(dgate_ref)

    stacked = stack_rows(rets, rows)
    first, second = dot_nn(hot_a[...], stacked), dot_nn(hot_b[...], stacked)
    dout = dout_ref[...].astype(F32)
    out_ref[...] = (in_ref[...].astype(F32) + (col(p_ref, 0) * first + col(p_ref, 1) * second)).astype(out_ref.dtype)
    for k, rows_k in enumerate((first, second)):
        dgate_ref[:, k * LANES:(k + 1) * LANES] += fold_lanes(rows_k * dout)

    if last:
        @pl.when(pl.program_id(0) == pl.num_programs(0) - 1)
        def _():
            p_a, p_b = col(p_ref, 0), col(p_ref, 1)
            g_a, g_b = lane_total(dgate_ref, 0), lane_total(dgate_ref, 1)
            mean = p_a * g_a + p_b * g_b
            expert = lax.broadcasted_iota(jnp.int32, dlog_ref.shape, 1)
            d_a = jnp.where(col(ids_ref, 0) == expert, p_a * (g_a - mean), 0.0)
            d_b = jnp.where(col(ids_ref, 1) == expert, p_b * (g_b - mean), 0.0)
            dlog_ref[...] = (d_a + d_b).astype(BF16)


def combine(tgt, gate_probs, dout, base, rets, first_slot, ids=None, dgates=None, experts=0, tile=512):
    tokens, dim = base.shape
    n_exp, cap, _ = rets[0].shape
    slots = len(rets) * n_exp * cap
    last = ids is not None
    full, cols, ret_spec = whole(tokens, 2), striped(tokens, tile), striped(n_exp, cap, tile)
    wide = whole(tokens, 2 * LANES)
    side = whole(tokens, experts) if last else wide
    side_shape = jax.ShapeDtypeStruct((tokens, experts), BF16) if last else jax.ShapeDtypeStruct((tokens, 2 * LANES), F32)
    return pl.pallas_call(
        functools.partial(combine_body, len(rets), first_slot, last),
        grid=(dim // tile,),
        in_specs=[full, full, cols, cols] + [ret_spec] * len(rets) + [full, wide] * last,
        out_specs=[cols, side],
        out_shape=[jax.ShapeDtypeStruct((tokens, dim), BF16 if last else F32), side_shape],
        scratch_shapes=[pltpu.VMEM((tokens, slots), BF16), pltpu.VMEM((tokens, slots), BF16), pltpu.VMEM((slots, tile), BF16)] + [pltpu.VMEM((tokens, 2 * LANES), F32)] * last,
        compiler_params=params(1),
        cost_estimate=cost(4 * tokens * slots * dim, 2 * (4 * tokens + slots) * dim),
        name="combine",
    )(tgt, gate_probs, dout, base, *rets, *((ids, dgates) if last else ()))


def near_body(n_ret, tgt_ref, *refs):
    rets, (out_ref, hot, rows) = refs[:n_ret], refs[n_ret:]

    @pl.when(pl.program_id(0) == 0)
    def _():
        fill_hot(tgt_ref, 0, hot)

    out_ref[...] = dot_nn(hot[...], stack_rows(rets, rows))


def near_rows(tgt, rets, tile=512):
    tokens = tgt.shape[0]
    n_exp, cap, dim = rets[0].shape
    slots = len(rets) * n_exp * cap
    return pl.pallas_call(
        functools.partial(near_body, len(rets)),
        grid=(dim // tile,),
        in_specs=[whole(tokens, 2)] + [striped(n_exp, cap, tile)] * len(rets),
        out_specs=striped(tokens, tile),
        out_shape=jax.ShapeDtypeStruct((tokens, dim), F32),
        scratch_shapes=[pltpu.VMEM((tokens, slots), BF16), pltpu.VMEM((slots, tile), BF16)],
        compiler_params=params(1),
        cost_estimate=cost(2 * tokens * slots * dim, 2 * (2 * tokens + slots) * dim),
        name="near_rows",
    )(tgt, *rets)


def finish_body(n_ret, first_slot, tgt_ref, dlog_ref, stat_ref, router_ref, gain_ref, x_ref, dout_ref, near_ref, *refs):
    rets = refs[:n_ret]
    gx_ref, ggain_ref, gbias_ref, hot, rows, d_hid, row_sums, means = refs[n_ret:]
    phase, n = pl.program_id(0), pl.program_id(1)
    tile = rets[0].shape[2]
    dim = d_hid.shape[1]
    cols = pl.ds(pl.multiple_of(n * tile, tile), tile)

    @pl.when((phase == 0) & (n == 0))
    def _():
        fill_hot(tgt_ref, first_slot, hot)
        row_sums[...] = jnp.zeros_like(row_sums)

    inv_std = col(stat_ref, 1)
    normed = (x_ref[...].astype(F32) - col(stat_ref, 0)) * inv_std

    @pl.when(phase == 0)
    def _():
        far = dot_nn(hot[...], stack_rows(rets, rows))
        rounded = (near_ref[...] + far + dot_nn(dlog_ref[...], router_ref[...])).astype(BF16)
        d_hid[:, cols] = rounded
        d_h = rounded.astype(F32)
        weighted = d_h * normed
        ggain_ref[...] = jnp.sum(weighted, axis=0, keepdims=True)
        gbias_ref[...] = jnp.sum(d_h, axis=0, keepdims=True)
        for k, rows_k in enumerate((d_h, weighted)):
            row_sums[:, k * LANES:(k + 1) * LANES] += fold_lanes(rows_k * gain_ref[...])

    @pl.when((phase == 1) & (n == 0))
    def _():
        for k in range(2):
            means[:, k:k + 1] = lane_total(row_sums, k) * (1.0 / dim)

    @pl.when(phase == 1)
    def _():
        d_norm = d_hid[:, cols].astype(F32) * gain_ref[...]
        mean_dn, mean_dnn = col(means, 0), col(means, 1)
        gx_ref[...] = (dout_ref[...].astype(F32) + inv_std * (d_norm - mean_dn - normed * mean_dnn)).astype(BF16)


def finish(tgt, d_logits, stats, router_t, gain, x_loc, dout, near, rets, first_slot, tile=512):
    tokens, dim = x_loc.shape
    experts = d_logits.shape[1]
    n_exp, cap, _ = rets[0].shape
    slots = len(rets) * n_exp * cap
    last = dim // tile - 1

    def early(p, n):
        return jnp.where(p == 0, n, last)

    full = whole(tokens, 2)
    both = pl.BlockSpec((tokens, tile), lambda p, n: (0, n))
    late = pl.BlockSpec((tokens, tile), lambda p, n: (0, n * p))
    line = pl.BlockSpec((1, tile), lambda p, n: (0, n))
    early_line = pl.BlockSpec((1, tile), lambda p, n: (0, early(p, n)))
    ret_spec = pl.BlockSpec((n_exp, cap, tile), lambda p, n: (0, 0, early(p, n)))
    return pl.pallas_call(
        functools.partial(finish_body, len(rets), first_slot),
        grid=(2, dim // tile),
        in_specs=[full, whole(tokens, experts), full, pl.BlockSpec((experts, tile), lambda p, n: (0, n)), line, both, late]
        + [pl.BlockSpec((tokens, tile), lambda p, n: (0, early(p, n)))] + [ret_spec] * len(rets),
        out_specs=[late, early_line, early_line],
        out_shape=[jax.ShapeDtypeStruct((tokens, dim), BF16), jax.ShapeDtypeStruct((1, dim), F32), jax.ShapeDtypeStruct((1, dim), F32)],
        scratch_shapes=[pltpu.VMEM((tokens, slots), BF16), pltpu.VMEM((slots, tile), BF16), pltpu.VMEM((tokens, dim), BF16), pltpu.VMEM((tokens, 2 * LANES), F32), pltpu.VMEM((tokens, 2), F32)],
        compiler_params=params(2),
        cost_estimate=cost(2 * tokens * slots * dim, 2 * (7 * tokens + slots) * dim),
        name="finish",
    )(tgt, d_logits, stats, router_t, gain, x_loc, dout, near, *rets)


def solution(mesh):
    n_dp, n_ep = mesh.shape["dp"], mesh.shape["ep"]
    tok_spec = P(("dp", "ep"), None)
    exp_spec = P("ep", None, None)

    def swap(value, bits):
        return lax.ppermute(value, "ep", [(j, j ^ bits) for j in range(n_ep)])

    def cross(value):
        return lax.ppermute(value, "dp", [(i, i ^ 1) for i in range(n_dp)])

    def total(value):
        value = value + swap(value, 1)
        value = value + cross(value)
        return value + swap(value, 2)

    def total_at_once(value):
        n_all = n_dp * n_ep
        parts = [value] + [lax.ppermute(value, ("dp", "ep"), [(d, d ^ k) for d in range(n_all)]) for k in range(1, n_all)]
        while len(parts) > 1:
            parts = [a + b for a, b in zip(parts[::2], parts[1::2])]
        return parts[0]

    def local_step(x_loc, ln_gain, ln_bias, w_router, w_gate, w_up, w_down, ids_loc, slots_loc, dout):
        tokens, dim = x_loc.shape
        experts = w_router.shape[1]
        n_exp = w_gate.shape[0]
        cap = capacity_for(tokens, experts, ids_loc.shape[1])
        local = n_exp * cap
        j = lax.axis_index("ep")
        gate_t, up_t = jnp.swapaxes(w_gate, 1, 2), jnp.swapaxes(w_up, 1, 2)
        base = (j * local).astype(jnp.int32)[None]

        def gather(routes, sources, scaled=False):
            rows, *hot = gather_call(True, scaled, sources, n_exp, cap, (base,) + routes)
            return rows, hot

        def gather_more(hot, sources, scaled=True):
            return gather_call(False, scaled, sources, n_exp, cap, hot)

        hidden, stats, logits = norm_router(x_loc, ln_gain[None], ln_bias[None], w_router.T)
        h_x, h_c, g_0 = swap(hidden, 2), swap(hidden, 1), cross(hidden)

        ids_t, slots_t, logits_t = ids_loc.T, slots_loc.T, logits.T
        kept = slots_t >= 0
        target = jnp.where(kept, ids_t * cap + slots_t, -1)
        picked = jnp.sum(jnp.where(ids_t[:, None, :] == jnp.arange(experts)[None, :, None], logits_t[None], 0.0), axis=1)
        probs = jax.nn.softmax(picked, axis=0)
        route = jnp.concatenate([target.astype(F32), probs, jnp.zeros((4, tokens), F32)])
        r_x, r_c, r_0 = swap(route, 2), swap(route, 1), cross(route)
        chunks = [(dim // 4 * s, dim // 4 * w) for s, w in ((0, 2), (2, 1), (3, 1))]
        d_cols = [lax.slice_in_dim(dout, s, s + w, axis=1) for s, w in chunks]
        d_x = [swap(part, 2) for part in d_cols]
        d_c, e_0 = swap(dout, 1), cross(dout)

        rows_a, hot_a = gather((route, r_c), (hidden, h_c))
        act_a = expert_forward(rows_a, gate_t, up_t, w_down)
        grads_a = gather_more(hot_a, (dout, d_c))
        back_a = expert_backward(grads_a, act_a[0], act_a[1], w_down, (gate_t, up_t))
        y_c = swap(act_a[4], 1)
        d_rows_c = swap(back_a[3], 1)
        tgt = jnp.where(kept, (ids_t // n_exp ^ j) * local + (ids_t % n_exp) * cap + slots_t, -1).T
        p_cols = probs.T
        moe_near, dgate_near = combine(tgt, p_cols, dout, x_loc, (act_a[3], y_c), 0)
        d_near = near_rows(tgt, (back_a[2], d_rows_c))

        h_xc, r_xc = swap(h_x, 1), swap(r_x, 1)
        g_2, r_2 = cross(h_x), cross(r_x)
        rows_b, hot_b = gather((r_x, r_xc), (h_x, h_xc))
        act_b = expert_forward(rows_b, gate_t, up_t, w_down)
        y_home = (swap(act_b[3], 2), swap(act_b[4], 3))

        grads_b, d_mix, e_2 = [], None, []
        for c, (start, width) in enumerate(chunks):
            grads_b.append(gather_more(hot_b, (d_x[c], swap(d_x[c], 1))))
            e_2.append(cross(d_x[c]))
            if c < len(chunks) - 1:
                d_mix = backward_chunk(grads_b[c], start, w_down, d_mix)
            else:
                back_b = expert_backward(grads_b[c], act_b[0], act_b[1], w_down, (gate_t, up_t), start, d_mix)
        d_home = (swap(back_b[2], 2), swap(back_b[3], 3))

        g_1, r_1, e_1 = swap(g_0, 1), swap(r_0, 1), swap(e_0, 1)
        grads_o, hot_o = gather((r_0, r_1), (e_0, e_1), True)
        rows_o = gather_more(hot_o, (g_0, g_1), False)
        act_o = expert_forward(rows_o, gate_t, up_t)

        back_o = expert_backward(grads_o, act_o[0], act_o[1], w_down)
        grad_gate = weight_grad((back_a[0], back_b[0], back_o[0]), (rows_a, rows_b, rows_o))
        parts = (back_a[1], back_b[1], back_o[1]), (rows_a, rows_b, rows_o)
        grad_up = weight_grad(*parts, None, False, 0, dim // 2)
        grad_up = weight_grad(*parts, grad_up, False, dim // 2, dim // 2)

        g_3, r_3 = swap(g_2, 1), swap(r_2, 1)
        rows_q, hot_q = gather((r_2, r_3), (g_2, g_3))
        act_q = expert_forward(rows_q, gate_t, up_t)

        moe_out, d_logits = combine(tgt, p_cols, dout, moe_near, y_home, 2 * local, ids_loc, dgate_near, experts)
        grad_router = total(jnp.einsum("te,tm->em", d_logits, hidden, preferred_element_type=F32))

        grad_down, d_mix = None, None
        for c, (start, width) in enumerate(chunks):
            e_3 = swap(e_2[c], 1)
            grads_q = gather_more(hot_q, (e_2[c], e_3))
            if c < len(chunks) - 1:
                d_mix = backward_chunk(grads_q, start, w_down, d_mix)
            else:
                back_q = expert_backward(grads_q, act_q[0], act_q[1], w_down, (), start, d_mix)
            grad_down = weight_grad((act_a[2], act_b[2], act_o[2], act_q[2]), (grads_a, grads_b[c], grads_o, grads_q), grad_down, False, start, width)
        grad_gate = weight_grad((back_q[0],), (rows_q,), grad_gate, True)
        grad_up = weight_grad((back_q[1],), (rows_q,), grad_up, True)

        grad_x, g_gain, g_bias = finish(tgt, d_logits, stats, w_router.T, ln_gain[None], x_loc, dout, d_near, d_home, 2 * local)
        g_norm = total_at_once(jnp.concatenate([g_gain, g_bias]))
        return (moe_out, grad_x, g_norm[0], g_norm[1], grad_router.T, jnp.swapaxes(grad_gate, 1, 2), jnp.swapaxes(grad_up, 1, 2), grad_down)

    return jax.shard_map(local_step, mesh=mesh, in_specs=(tok_spec, P(None), P(None), P(None, None), exp_spec, exp_spec, exp_spec, tok_spec, tok_spec, tok_spec), out_specs=(tok_spec, tok_spec, P(None), P(None), P(None, None), exp_spec, exp_spec, exp_spec), check_vma=False)
```
